256 devices in a mesh: gz: 32 (over y_lo, z, core), xy: 8 (over x, y_hi).
Axes of the slice: x: 4, y: 4 (y_hi: 2, y_lo: 2; y = y_hi * 2 + y_lo), z: 8, core: 2. Of those that a mesh axis runs over, the one named last changes fastest.
Arguments:
- fields: float32 [2, 2048, 256, 256], P(None, 'gz', 'xy'), may hold values from -64 to 64, as said below
- threshold: float32 [2], replicated, may hold values from 0.1 to 0.6
Outputs:
- detail_one: float32 [2, 1024, 256, 256], P(None, 'gz', 'xy')
- detail_two: float32 [2, 512, 256, 256], P(None, 'gz', 'xy')
- detail_three: float32 [2, 256, 256, 256], P(None, 'gz', 'xy')
- detail_four: float32 [2, 128, 256, 256], P(None, 'gz', 'xy')
- detail_five: float32 [2, 64, 256, 256], P(None, 'gz', 'xy')
- coarse: float32 [2, 64, 256, 256], P(None, 'gz', 'xy')
- band_energy: float32 [2, 6], replicated
The draws below stay inside these ranges and needn't reach their ends.
Inputs may be any that keep to these rules, and one draw needn't show every extreme that they name: Finite values; the spread of the fields varies over the grid.
All inputs are finite; a program needn't handle non-finite values.
Results may differ from the reference program's by a relative error of at most 0.00002.
Values sent between devices are 32-bit elements; how exact they have to be, the bound alone decides.
No kernel may reach another device: no remote copies, remote signals or barrier semaphores. Data moves between devices by JAX's collectives and lax.ppermute only.
A program may use at most 64 MiB of HBM per device.

```python
import jax
import jax.numpy as jnp

NY = 256
NZ = 2048
NX = 256


def draw_fields(key, part):
    depth = jnp.arange(NZ, dtype=jnp.float32) / NZ
    across = jnp.arange(NX, dtype=jnp.float32) / NX
    scale = jnp.exp(jnp.log(4.0) * depth)[:, None, None] * (1.0 + across)[None, :, None]
    noise = jax.random.normal(jax.random.fold_in(key, 13), (2, NZ, NX, NY), jnp.float32)
    values = noise * scale[None]
    return values.astype(jnp.float32)


def setup_inputs(seed: int = 0) -> dict:
    key_of = jax.random.split(jax.random.key(seed), 3)
    return {
        "fields": draw_fields(jax.random.fold_in(key_of[2], 71), 0),
        "threshold": jnp.clip(jax.random.uniform(key_of[1], (2,), jnp.float32, 0.1, 0.6), 0.1, 0.6),
    }


ALPHA = -1.586134342059924
BETA = -0.052980118572961
GAMMA = 0.882911075530934
DELTA = 0.443506852043971
KAPPA = 1.230174104914001
SQRT_TWO = 1.4142135623730951


def right_of(evens):
    return jnp.concatenate([evens[:, 1:], evens[:, -1:]], axis=1)


def left_of(odds):
    return jnp.concatenate([odds[:, :1], odds[:, :-1]], axis=1)


def one_level(values):
    half = values.shape[1] // 2
    paired = values.reshape(values.shape[0], half, 2, values.shape[2], values.shape[3])
    evens = paired[:, :, 0]
    odds = paired[:, :, 1]
    odds = odds + ALPHA * (evens + right_of(evens))
    evens = evens + BETA * (left_of(odds) + odds)
    odds = odds + GAMMA * (evens + right_of(evens))
    evens = evens + DELTA * (left_of(odds) + odds)
    return evens * (SQRT_TWO / KAPPA), odds * (KAPPA / SQRT_TWO)


def shrink(band, limit):
    return band - jnp.clip(band, -limit, limit)


def reference(fields, threshold):
    limit = threshold.reshape(2, 1, 1, 1)
    bands = []
    approx = fields
    for level in range(5):
        approx, detail = one_level(approx)
        bands.append(shrink(detail, limit))
    bands.append(shrink(approx, limit))
    energy = jnp.stack([jnp.sum(band * band, axis=(1, 2, 3)) / (band.shape[1] * band.shape[2] * band.shape[3]) for band in bands], axis=1)
    return (bands[0], bands[1], bands[2], bands[3], bands[4], bands[5], energy)
```

```python
import functools

import jax
import jax.numpy as jnp
import numpy as np
from jax import lax
from jax.experimental import pallas as pl
from jax.experimental.pallas import tpu as pltpu
from jax.sharding import PartitionSpec as P

ALPHA = -1.586134342059924
BETA = -0.052980118572961
GAMMA = 0.882911075530934
DELTA = 0.443506852043971
KAPPA = 1.230174104914001
SQRT_TWO = 1.4142135623730951
LOW = SQRT_TWO / KAPPA
HIGH = KAPPA / SQRT_TWO
FAR = 4
EDGE_LO = (1, 2, 3, 3)
EDGE_HI = (2, 3, 3, 3)


class Level:
    def __init__(self, n, left, right, emit_d, emit_s):
        self.n, self.left, self.right, self.emit_d, self.emit_s = n, left, right, emit_d, emit_s
        self.s, self.d, self.d1, self.s2, self.d3 = [], [], [], [], []

    def push(self, x):
        if len(self.s) == len(self.d):
            self.s.append(x)
            i = len(self.s) - 2
            if i >= 0:
                self.add(self.d[i] + ALPHA * (self.s[i] + self.s[i + 1]))
        else:
            self.d.append(x)
            if len(self.d) == self.n:
                self.finish()

    def add(self, v):
        self.d1.append(v)
        i = len(self.d1) - 1
        if i == 0:
            self.p = ALPHA * self.s[0]
            self.c = self.s[0] + BETA * v
            return
        if i == 1:
            a, b = self.left(self)
            below = a + self.p
            self.s2.append(self.c + BETA * below)
            self.d3m = below + GAMMA * ((b + BETA * below) + self.s2[0])
        if i == self.n - 1:
            self.s2.append(self.b + BETA * v)
        else:
            self.s2.append(self.s[i] + BETA * (self.d1[i - 1] + v))
        self.third(i - 1, self.s2[i])

    def third(self, j, above):
        self.d3.append(self.d1[j] + GAMMA * (self.s2[j] + above))
        self.emit_d(j, self.d3[j])
        before = self.d3[j - 1] if j else self.d3m
        self.emit_s(j, self.s2[j] + DELTA * (before + self.d3[j]))

    def finish(self):
        n = self.n
        self.a = self.d[n - 1] + ALPHA * self.s[n - 1]
        self.b = self.s[n - 1] + BETA * self.d1[n - 2]
        p, c = self.right(self)
        v = self.a + p
        self.add(v)
        self.third(n - 1, c + BETA * v)


def low_end(level):
    return level.d[0] + ALPHA * level.s[1], level.s[1] + BETA * level.d1[1]


def high_end(level):
    return ALPHA * level.s[-1], level.b


@functools.cache
def response(side):
    width = 2 * FAR
    zero, unit = np.zeros(width), np.eye(width)
    back, details, u = [], [], [zero] * 512
    for l in range(FAR):
        n = len(u) // 2
        state, none = (unit[2 * l], unit[2 * l + 1]), (zero, zero)
        d, s = [None] * n, [None] * n
        level = Level(
            n,
            lambda _: state if side == "lo" else none,
            lambda _: state if side == "hi" else none,
            d.__setitem__,
            s.__setitem__,
        )
        for x in u:
            level.push(x)
        back.append((level.p, level.c) if side == "lo" else (level.a, level.b))
        details.append(d[:6] if side == "lo" else d[::-1][:6])
        last = s[:6] if side == "lo" else s[::-1][:6]
        u = s
    return back, details, last


def combine(row, states):
    total = None
    for k, x in zip(row, states):
        if k != 0.0:
            term = float(k) * x
            total = term if total is None else total + term
    return total


def where_am_i():
    z = lax.axis_index("gz")
    return lax.rem(z, 2) == 1, z == 0, z == lax.axis_size("gz") - 1


def cell(i):
    return i // 8, pl.ds(pl.multiple_of(lax.rem(i // 2, 4) * 8, 8), 8), pl.ds(pl.multiple_of(lax.rem(i, 2) * 128, 128), 128)


def transform(x_hbm, outer, inner, d1, d2, d3, d4, s4, x_vmem, sem):
    upper, lowest, highest = where_am_i()

    def fetch(j):
        rows = pl.ds(pl.multiple_of(lax.rem(j, 4) * 8, 8), 8)
        at = (j // 4, slice(None), rows)
        return pltpu.make_async_copy(x_hbm.at[at], x_vmem.at[at], sem.at[j])

    for j in range(8):
        fetch(j).start()
    from_above, from_below = response("hi")[0], response("lo")[0]
    bands = (d1, d2, d3, d4)

    def tile(i, _):
        @pl.when(lax.rem(i, 2) == 0)
        def _():
            fetch(i // 2).wait()

        f, rows, cols = cell(i)
        down, up, levels = [], [], []

        def left(l):
            def state(level):
                down.extend((level.p, level.c))
                end = low_end(level)
                if l == 0:
                    return tuple(jnp.where(lowest, e, 0.0) for e in end)
                return tuple(jnp.where(lowest, e, combine(r, down)) for e, r in zip(end, from_above[l]))

            return state

        def right(l):
            def state(level):
                up.extend((level.a, level.b))
                end = high_end(level)
                if l == 0:
                    return tuple(jnp.where(highest, e, 0.0) for e in end)
                return tuple(jnp.where(highest, e, combine(r, up)) for e, r in zip(end, from_below[l]))

            return state

        def keep(l):
            def store(j, v):
                bands[l][f, j, rows, cols] = v

            return store

        def pass_on(l):
            def store(j, v):
                if l == FAR - 1:
                    s4[f, j, rows, cols] = v
                else:
                    levels[l + 1].push(v)

            return store

        for l in range(FAR):
            levels.append(Level(32 >> l, left(l), right(l), keep(l), pass_on(l)))
        for z in range(64):
            levels[0].push(x_vmem[f, z, rows, cols])
        for k in range(2 * FAR):
            outer[f, k, rows, cols] = jnp.where(upper, up[k], down[k])
            inner[f, k, rows, cols] = jnp.where(upper, down[k], up[k])
        return 0

    lax.fori_loop(0, 16, tile, 0)


def shrink(v, scale, limit):
    v = v * scale
    return v - jnp.clip(v, -limit, limit)


def interiors(limits, d1, d2, d3, o1, o2, o3, sums, b1, b2, b3, sem):
    copies = []
    for f in range(2):
        limit = limits[f]
        for l, (raw, buf, out) in enumerate(((d1, b1, o1), (d2, b2, o2), (d3, b3, o3))):
            n = 32 >> l
            lo, hi = EDGE_LO[l], n - EDGE_HI[l]

            def layer(z, acc, raw=raw, buf=buf, l=l):
                v = shrink(raw[f, z], LOW**l * HIGH, limit)
                buf[f, z] = v
                return acc + v * v

            acc = lax.fori_loop(lo, hi, layer, jnp.zeros((32, 256), jnp.float32), unroll=True)
            acc = acc.reshape(4, 8, 256).sum(axis=0)
            sums[f, l] = acc[:, :128] + acc[:, 128:]
            at = (f, pl.ds(lo, hi - lo))
            copy = pltpu.make_async_copy(buf.at[at], out.at[at], sem.at[3 * f + l])
            copy.start()
            copies.append(copy)
    for copy in copies:
        copy.wait()


def arrived(outer, inner, f, rows, cols, upper, lowest, highest, width):
    below, above = [], []
    for k in range(width):
        o, i = outer[f, k, rows, cols], inner[f, k, rows, cols]
        below.append(jnp.where(lowest, 0.0, jnp.where(upper, i, o)))
        above.append(jnp.where(highest, 0.0, jnp.where(upper, o, i)))
    return below, above


def corrected(v, row_lo, below, row_hi, above):
    for term in (combine(row_lo, below), combine(row_hi, above)):
        if term is not None:
            v = v + term
    return v


def approximation(outer, inner, s4, outer5, inner5, full):
    upper, lowest, highest = where_am_i()
    last_lo, last_hi = response("lo")[2], response("hi")[2]

    def tile(i, _):
        f, rows, cols = cell(i)
        below, above = arrived(outer, inner, f, rows, cols, upper, lowest, highest, 2 * FAR)
        u = [corrected(s4[f, j, rows, cols], last_lo[j], below, last_hi[3 - j], above) for j in range(4)]
        for j in range(4):
            full[f, j, rows, cols] = u[j]
        middle = u[1] + ALPHA * (u[0] + u[2])
        down = (ALPHA * u[0], u[0] + BETA * middle)
        up = (u[3] + ALPHA * u[2], u[2] + BETA * middle)
        for k in range(2):
            outer5[f, k, rows, cols] = jnp.where(upper, up[k], down[k])
            inner5[f, k, rows, cols] = jnp.where(upper, down[k], up[k])
        return 0

    lax.fori_loop(0, 16, tile, 0)


def edges(limits, outer, inner, d1, d2, d3, d4, o1_in, o2_in, o3_in, o1, o2, o3, o4, sums, b1, b2, b3, b4, sem):
    upper, lowest, highest = where_am_i()
    det_lo, det_hi = response("lo")[1], response("hi")[1]
    raws, bufs, outs = (d1, d2, d3, d4), (b1, b2, b3, b4), (o1, o2, o3, o4)
    spans = [sorted({*range(EDGE_LO[l]), *range((32 >> l) - EDGE_HI[l], 32 >> l)}) for l in range(FAR)]
    sums[...] = jnp.zeros(sums.shape, jnp.float32)

    def tile(i, _):
        f, rows, cols = cell(i)
        limit = limits[f]
        below, above = arrived(outer, inner, f, rows, cols, upper, lowest, highest, 2 * FAR)
        for l in range(FAR):
            n, acc = 32 >> l, None
            for k, j in enumerate(spans[l]):
                row_lo = det_lo[l][j] if j < 6 else ()
                row_hi = det_hi[l][n - 1 - j] if n - 1 - j < 6 else ()
                v = corrected(raws[l][f, j, rows, cols], row_lo, below, row_hi, above)
                v = shrink(v, LOW**l * HIGH, limit)
                bufs[l][f, k, rows, cols] = v
                acc = v * v if acc is None else acc + v * v
            sums[f, l] += acc
        return 0

    lax.fori_loop(0, 16, tile, 0)
    copies = []
    for f in range(2):
        for l in range(FAR):
            n, lo = 32 >> l, EDGE_LO[l]
            pieces = [(0, lo, 0), (lo, len(spans[l]) - lo, n - EDGE_HI[l])] if l < 3 else [(0, n, 0)]
            for start, size, to in pieces:
                copy = pltpu.make_async_copy(
                    bufs[l].at[f, pl.ds(start, size)], outs[l].at[f, pl.ds(to, size)], sem.at[len(copies)]
                )
                copy.start()
                copies.append(copy)
    for copy in copies:
        copy.wait()


def fifth(limits, outer, inner, full, sums_a, sums_b, o5, o6, total, b5, b6, acc, sem):
    upper, lowest, highest = where_am_i()
    acc[...] = jnp.zeros(acc.shape, jnp.float32)

    def tile(i, _):
        f, rows, cols = cell(i)
        limit = limits[f]
        below, above = arrived(outer, inner, f, rows, cols, upper, lowest, highest, 2)

        def left(level):
            return tuple(jnp.where(lowest, e, v) for e, v in zip(low_end(level), below))

        def right(level):
            return tuple(jnp.where(highest, e, v) for e, v in zip(high_end(level), above))

        def keep_d(j, v):
            v = shrink(v, LOW**4 * HIGH, limit)
            b5[f, j, rows, cols] = v
            acc[f, 0] += v * v

        def keep_s(j, v):
            v = shrink(v, LOW**5, limit)
            b6[f, j, rows, cols] = v
            acc[f, 1] += v * v

        level = Level(2, left, right, keep_d, keep_s)
        for j in range(4):
            level.push(full[f, j, rows, cols])
        return 0

    lax.fori_loop(0, 16, tile, 0)
    copies = [pltpu.make_async_copy(b5, o5, sem.at[0]), pltpu.make_async_copy(b6, o6, sem.at[1])]
    for copy in copies:
        copy.start()
    lane = lax.broadcasted_iota(jnp.int32, (1, 128), 1)
    row = jnp.zeros((1, 128), jnp.float32)
    for f in range(2):
        for b in range(6):
            if b < 3:
                part = sums_a[f, b] + sums_b[f, b]
            elif b < 4:
                part = sums_b[f, b]
            else:
                part = acc[f, b - 4]
            row = row + jnp.where(lane == 6 * f + b, jnp.sum(part), 0.0)
    total[...] = row
    for copy in copies:
        copy.wait()


def local(fields, threshold):
    f32 = jnp.float32
    vmem, hbm, smem = (pl.BlockSpec(memory_space=m) for m in (pltpu.VMEM, pltpu.HBM, pltpu.SMEM))

    def arr(n):
        return jax.ShapeDtypeStruct((2, n, 32, 256), f32)

    def buf(n):
        return pltpu.VMEM((2, n, 32, 256), f32)

    def call(body, ins, outs, scratch, name, flops, mib, aliases=None):
        return pl.pallas_call(
            body,
            in_specs=ins,
            out_specs=[s for s, _ in outs],
            out_shape=[a for _, a in outs],
            scratch_shapes=scratch,
            input_output_aliases=aliases or {},
            compiler_params=pltpu.CompilerParams(vmem_limit_bytes=mib << 20),
            cost_estimate=pl.CostEstimate(flops=flops, bytes_accessed=1 << 20, transcendentals=0),
            name=name,
        )

    count = lax.axis_size("gz")
    across = [(i, (i + 1) % count if i % 2 else (i - 1) % count) for i in range(count)]
    within = [(i, i ^ 1) for i in range(count)]

    outer, inner, d1, d2, d3, d4, s4 = call(
        transform,
        [hbm],
        [(vmem, arr(8)), (vmem, arr(8)), (vmem, arr(32)), (vmem, arr(16)), (vmem, arr(8)), (vmem, arr(4)), (vmem, arr(4))],
        [buf(64), pltpu.SemaphoreType.DMA((8,))],
        "transform",
        20_000_000,
        8,
    )(fields)
    outer = lax.ppermute(outer, "gz", across)
    inner = lax.ppermute(inner, "gz", within)
    o1, o2, o3, sums_a = call(
        interiors,
        [smem, vmem, vmem, vmem],
        [(hbm, arr(32)), (hbm, arr(16)), (hbm, arr(8)), (vmem, jax.ShapeDtypeStruct((2, 3, 8, 128), f32))],
        [buf(32), buf(16), buf(8), pltpu.SemaphoreType.DMA((6,))],
        "interiors",
        2_000_000_000,
        8,
    )(threshold, d1, d2, d3)
    outer5, inner5, full = call(
        approximation,
        [vmem] * 3,
        [(vmem, arr(2)), (vmem, arr(2)), (vmem, arr(4))],
        [],
        "approximation",
        5_000_000,
        4,
    )(outer, inner, s4)
    outer5 = lax.ppermute(outer5, "gz", across)
    inner5 = lax.ppermute(inner5, "gz", within)
    o1, o2, o3, o4, sums_b = call(
        edges,
        [smem] + [vmem] * 6 + [hbm] * 3,
        [(hbm, arr(32)), (hbm, arr(16)), (hbm, arr(8)), (hbm, arr(4)), (vmem, jax.ShapeDtypeStruct((2, 4, 8, 128), f32))],
        [buf(3), buf(5), buf(6), buf(4), pltpu.SemaphoreType.DMA((14,))],
        "edges",
        1_000_000_000,
        6,
        {7: 0, 8: 1, 9: 2},
    )(threshold, outer, inner, d1, d2, d3, d4, o1, o2, o3)
    o5, o6, total = call(
        fifth,
        [smem] + [vmem] * 5,
        [(hbm, arr(2)), (hbm, arr(2)), (vmem, jax.ShapeDtypeStruct((1, 128), f32))],
        [buf(2), buf(2), pltpu.VMEM((2, 2, 8, 128), f32), pltpu.SemaphoreType.DMA((2,))],
        "fifth",
        5_000_000,
        4,
    )(threshold, outer5, inner5, full, sums_a, sums_b)

    devices = count * lax.axis_size("xy")
    parts = lax.all_to_all(jnp.broadcast_to(total[:, :12], (devices, 12)), ("gz", "xy"), 0, 0, tiled=True)
    cells = np.array([n * 32 * 256 * devices for n in (32, 16, 8, 4, 2, 2)] * 2, np.float32)
    energy = (jnp.sum(parts, axis=0) / cells).reshape(2, 6)
    return o1, o2, o3, o4, o5, o6, energy


def solution(mesh):
    split = P(None, "gz", "xy", None)
    return jax.shard_map(local, mesh=mesh, in_specs=(split, P()), out_specs=(split,) * 6 + (P(),), check_vma=False)
```

```python
import functools

import jax
import jax.numpy as jnp
import numpy as np
from jax import lax
from jax.experimental import pallas as pl
from jax.experimental.pallas import tpu as pltpu
from jax.sharding import PartitionSpec as P

ALPHA = -1.586134342059924
BETA = -0.052980118572961
GAMMA = 0.882911075530934
DELTA = 0.443506852043971
KAPPA = 1.230174104914001
SQRT_TWO = 1.4142135623730951
LOW = SQRT_TWO / KAPPA
HIGH = KAPPA / SQRT_TWO
LEVELS = 5
FAR = 8
ALL = 2 * LEVELS
EDGE_LO = (1, 2, 3)
EDGE_HI = (2, 3, 3)
SPANS = [sorted({*range(lo), *range((32 >> l) - hi, 32 >> l)}) for l, (lo, hi) in enumerate(zip(EDGE_LO, EDGE_HI))]
SPANS += [[0, 1, 2, 3]]


class Level:
    def __init__(self, n, left, right, emit_d, emit_s):
        self.n, self.left, self.right, self.emit_d, self.emit_s = n, left, right, emit_d, emit_s
        self.s, self.d, self.d1, self.s2, self.d3 = [], [], [], [], []

    def push(self, x):
        if len(self.s) == len(self.d):
            self.s.append(x)
            i = len(self.s) - 2
            if i >= 0:
                self.add(self.d[i] + ALPHA * (self.s[i] + self.s[i + 1]))
        else:
            self.d.append(x)
            if len(self.d) == self.n:
                self.finish()

    def add(self, v):
        self.d1.append(v)
        i = len(self.d1) - 1
        if i == 0:
            self.p = ALPHA * self.s[0]
            self.c = self.s[0] + BETA * v
            return
        if i == 1:
            a, b = self.left(self)
            below = a + self.p
            self.s2.append(self.c + BETA * below)
            self.d3m = below + GAMMA * ((b + BETA * below) + self.s2[0])
        if i == self.n - 1:
            self.s2.append(self.b + BETA * v)
        else:
            self.s2.append(self.s[i] + BETA * (self.d1[i - 1] + v))
        self.third(i - 1, self.s2[i])

    def third(self, j, above):
        self.d3.append(self.d1[j] + GAMMA * (self.s2[j] + above))
        self.emit_d(j, self.d3[j])
        before = self.d3[j - 1] if j else self.d3m
        self.emit_s(j, self.s2[j] + DELTA * (before + self.d3[j]))

    def finish(self):
        n = self.n
        self.a = self.d[n - 1] + ALPHA * self.s[n - 1]
        self.b = self.s[n - 1] + BETA * self.d1[n - 2]
        p, c = self.right(self)
        v = self.a + p
        self.add(v)
        self.third(n - 1, c + BETA * v)


def low_end(level):
    return level.d[0] + ALPHA * level.s[1], level.s[1] + BETA * level.d1[1]


def high_end(level):
    return ALPHA * level.s[-1], level.b


@functools.cache
def response(side, length=1024):
    zero, unit = np.zeros(2 * LEVELS), np.eye(2 * LEVELS)
    found, u = [], [zero] * length
    for l in range(LEVELS):
        n = len(u) // 2
        state, none = (unit[2 * l], unit[2 * l + 1]), (zero, zero)
        d, s = [None] * n, [None] * n
        level = Level(
            n,
            lambda _: state if side == "lo" else none,
            lambda _: state if side == "hi" else none,
            d.__setitem__,
            s.__setitem__,
        )
        for x in u:
            level.push(x)
        u = s
        down, up = (level.p, level.c), (level.a, level.b)
        found.append((down, up, d, s) if side == "lo" else (up, down, d[::-1], s[::-1]))
    return found


TRANSFORM_MIB = 47
BACK, ON, DETAIL, APPROX = range(4)


def combine(row, states):
    total = None
    for k, x in zip(row, states):
        if k != 0.0:
            term = float(k) * x
            total = term if total is None else total + term
    return total


def where_am_i():
    z = lax.axis_index("gz")
    return lax.rem(z, 2) == 1, z == 0, z == lax.axis_size("gz") - 1


def cell(i):
    return i // 8, pl.ds(pl.multiple_of(lax.rem(i // 2, 4) * 8, 8), 8), pl.ds(pl.multiple_of(lax.rem(i, 2) * 128, 128), 128)


def transform(x_hbm, outer, outer5, inner, d1, d2, d3, d4, d5, s5, x_vmem, sem):
    upper, lowest, highest = where_am_i()

    def fetch(j):
        rows = pl.ds(pl.multiple_of(lax.rem(j, 4) * 8, 8), 8)
        at = (j // 4, slice(None), rows)
        return pltpu.make_async_copy(x_hbm.at[at], x_vmem.at[at], sem.at[j])

    for j in range(8):
        fetch(j).start()
    from_above, from_below = response("hi"), response("lo")
    bands = (d1, d2, d3, d4, d5)

    def tile(i, _):
        @pl.when(lax.rem(i, 2) == 0)
        def _():
            fetch(i // 2).wait()

        f, rows, cols = cell(i)
        down, up, levels = [], [], []

        def left(l):
            def state(level):
                down.extend((level.p, level.c))
                end = low_end(level)
                if l == 0:
                    return tuple(jnp.where(lowest, e, 0.0) for e in end)
                return tuple(jnp.where(lowest, e, combine(r, down)) for e, r in zip(end, from_above[l][BACK]))

            return state

        def right(l):
            def state(level):
                up.extend((level.a, level.b))
                end = high_end(level)
                if l == 0:
                    return tuple(jnp.where(highest, e, 0.0) for e in end)
                return tuple(jnp.where(highest, e, combine(r, up)) for e, r in zip(end, from_below[l][BACK]))

            return state

        def keep(l):
            def store(j, v):
                bands[l][f, j, rows, cols] = v

            return store

        def pass_on(l):
            def store(j, v):
                if l == LEVELS - 1:
                    s5[f, j, rows, cols] = v
                else:
                    levels[l + 1].push(v)

            return store

        for l in range(LEVELS):
            levels.append(Level(32 >> l, left(l), right(l), keep(l), pass_on(l)))
        for z in range(64):
            levels[0].push(x_vmem[f, z, rows, cols])
        for k in range(ALL):
            out = jnp.where(upper, up[k], down[k])
            if k < FAR:
                outer[f, k, rows, cols] = out
            else:
                outer5[f, k - FAR, rows, cols] = out
            inner[f, k, rows, cols] = jnp.where(upper, down[k], up[k])
        return 0

    lax.fori_loop(0, 16, tile, 0)


def shrink(v, scale, limit):
    v = v * scale
    return v - jnp.clip(v, -limit, limit)


def corrected(v, *parts):
    for row, states in parts:
        term = combine(row, states)
        if term is not None:
            v = term if v is None else v + term
    return v


def through(states, upper):
    lo, hi = response("lo", 64)[4][ON], response("hi", 64)[4][ON]
    sums = []
    for k in range(2):
        row = [jnp.where(upper, float(x), float(y)) for x, y in zip(lo[k], hi[k])]
        total = row[0] * states[0]
        for x, state in list(zip(row, states))[1:]:
            total = total + x * state
        sums.append(total)
    return sums


def hand_on(own5, inner, out5):
    upper, _, _ = where_am_i()

    def tile(i, _):
        f, rows, cols = cell(i)
        extra = through([inner[f, k, rows, cols] for k in range(FAR)], upper)
        for k in range(2):
            out5[f, k, rows, cols] = own5[f, k, rows, cols] + extra[k]
        return 0

    lax.fori_loop(0, 16, tile, 0)


def hand_in(outer, after, out5):
    upper, lowest, highest = where_am_i()
    end = jnp.logical_or(lowest, highest)

    def tile(i, _):
        f, rows, cols = cell(i)
        extra = through([outer[f, k, rows, cols] for k in range(FAR)], jnp.logical_not(upper))
        for k in range(2):
            out5[f, k, rows, cols] = jnp.where(end, 0.0, extra[k])
        return 0

    lax.fori_loop(0, 16, tile, 0)


def interiors(limits, d1, d2, d3, after, o1, o2, o3, sums, b1, b2, b3, sem):
    copies = []
    for f in range(2):
        limit = limits[f]
        for l, (raw, buf, out) in enumerate(((d1, b1, o1), (d2, b2, o2), (d3, b3, o3))):
            n = 32 >> l
            lo, hi = EDGE_LO[l], n - EDGE_HI[l]

            def layer(z, acc, raw=raw, buf=buf, l=l):
                v = shrink(raw[f, z], LOW**l * HIGH, limit)
                buf[f, z] = v
                return acc + v * v

            acc = lax.fori_loop(lo, hi, layer, jnp.zeros((32, 256), jnp.float32), unroll=True)
            acc = acc.reshape(4, 8, 256).sum(axis=0)
            sums[f, l] = acc[:, :128] + acc[:, 128:]
            at = (f, pl.ds(lo, hi - lo))
            copy = pltpu.make_async_copy(buf.at[at], out.at[at], sem.at[3 * f + l])
            copy.start()
            copies.append(copy)
    for copy in copies:
        copy.wait()


def arrived(outer, inner, f, rows, cols, upper, lowest, highest, width):
    below, above = [], []
    for k in range(width):
        o, i = outer[f, k, rows, cols], inner[f, k, rows, cols]
        below.append(jnp.where(lowest, 0.0, jnp.where(upper, i, o)))
        above.append(jnp.where(highest, 0.0, jnp.where(upper, o, i)))
    return below, above


def edges(limits, outer, inner, d1, d2, d3, d4, d5, s5, after, b1, b2, b3, b4, base, ends, sums):
    upper, lowest, highest = where_am_i()
    lo, hi = response("lo"), response("hi")
    pass_up = response("lo", 64)[4][ON]
    raws, bufs = (d1, d2, d3, d4), (b1, b2, b3, b4)
    sums[...] = jnp.zeros(sums.shape, jnp.float32)

    def tile(i, _):
        f, rows, cols = cell(i)
        limit = limits[f]
        below, above = arrived(outer, inner, f, rows, cols, upper, lowest, highest, FAR)
        for j in range(2):
            base[f, j, rows, cols] = corrected(
                d5[f, j, rows, cols], (lo[4][DETAIL][j][:FAR], below), (hi[4][DETAIL][1 - j][:FAR], above)
            )
            base[f, 2 + j, rows, cols] = corrected(
                s5[f, j, rows, cols], (lo[4][APPROX][j][:FAR], below), (hi[4][APPROX][1 - j][:FAR], above)
            )
            ends[f, j, rows, cols] = jnp.zeros((8, 128), jnp.float32)

        @pl.when(lowest)
        def _():
            u = [combine(hi[3][APPROX][3 - j], above) for j in range(4)]
            ends[f, 0, rows, cols] = u[1] + ALPHA * u[2]
            ends[f, 1, rows, cols] = u[2] + BETA * ((u[3] + ALPHA * u[2]) + inner[f, FAR, rows, cols])

        @pl.when(highest)
        def _():
            ends[f, 0, rows, cols] = ALPHA * combine(lo[3][APPROX][2], below)
            ends[f, 1, rows, cols] = combine(pass_up[1], below)

        for l in range(4):
            n, acc = 32 >> l, None
            for k, j in enumerate(SPANS[l]):
                row_lo = lo[l][DETAIL][j] if j < 6 else ()
                row_hi = hi[l][DETAIL][n - 1 - j] if n - 1 - j < 6 else ()
                v = corrected(raws[l][f, j, rows, cols], (row_lo, below), (row_hi, above))
                v = shrink(v, LOW**l * HIGH, limit)
                bufs[l][f, k, rows, cols] = v
                acc = v * v if acc is None else acc + v * v
            sums[f, l] += acc
        return 0

    lax.fori_loop(0, 16, tile, 0)


def fifth(limits, outer5, inner, relayed, base, ends, sums_a, sums_b, b5, b6, total, acc):
    upper, lowest, highest = where_am_i()
    lo, hi = response("lo")[4], response("hi")[4]
    acc[...] = jnp.zeros(acc.shape, jnp.float32)

    def tile(i, _):
        f, rows, cols = cell(i)
        limit = limits[f]
        below, above = [], []
        for k in range(2):
            o = outer5[f, k, rows, cols]
            n = inner[f, FAR + k, rows, cols] + relayed[f, k, rows, cols]
            e = ends[f, k, rows, cols]
            below.append(jnp.where(lowest, e, jnp.where(upper, n, o)))
            above.append(jnp.where(highest, e, jnp.where(upper, o, n)))
        for j in range(2):
            d = corrected(base[f, j, rows, cols], (lo[DETAIL][j][FAR:], below), (hi[DETAIL][1 - j][FAR:], above))
            d = shrink(d, LOW**4 * HIGH, limit)
            b5[f, j, rows, cols] = d
            s = corrected(base[f, 2 + j, rows, cols], (lo[APPROX][j][FAR:], below), (hi[APPROX][1 - j][FAR:], above))
            s = shrink(s, LOW**5, limit)
            b6[f, j, rows, cols] = s
            acc[f, 0] += d * d
            acc[f, 1] += s * s
        return 0

    lax.fori_loop(0, 16, tile, 0)
    lane = lax.broadcasted_iota(jnp.int32, (1, 128), 1)
    row = jnp.zeros((1, 128), jnp.float32)
    for f in range(2):
        for b in range(6):
            if b < 3:
                part = sums_a[f, b] + sums_b[f, b]
            elif b < 4:
                part = sums_b[f, b]
            else:
                part = acc[f, b - 4]
            row = row + jnp.where(lane == 6 * f + b, jnp.sum(part), 0.0)
    total[...] = row


def finish(cells, parts, b1, b2, b3, b4, b5, b6, o1_in, o2_in, o3_in, o1, o2, o3, o4, o5, o6, energy, sem):
    copies = []
    for f in range(2):
        for l, (buf, out) in enumerate(((b1, o1), (b2, o2), (b3, o3))):
            lo, hi, n = EDGE_LO[l], EDGE_HI[l], 32 >> l
            for start, size, to in ((0, lo, 0), (lo, hi, n - hi)):
                copies.append((buf.at[f, pl.ds(start, size)], out.at[f, pl.ds(to, size)]))
    copies += [(b4, o4), (b5, o5), (b6, o6)]
    copies = [pltpu.make_async_copy(a, b, sem.at[k]) for k, (a, b) in enumerate(copies)]
    for copy in copies:
        copy.start()
    row = jnp.sum(parts[...], axis=0) * (1.0 / cells[...])
    energy[0:1, :] = row[:, 0:6]
    energy[1:2, :] = row[:, 6:12]
    for copy in copies:
        copy.wait()


def local(fields, threshold):
    f32 = jnp.float32
    vmem, hbm, smem = (pl.BlockSpec(memory_space=m) for m in (pltpu.VMEM, pltpu.HBM, pltpu.SMEM))

    def arr(n):
        return jax.ShapeDtypeStruct((2, n, 32, 256), f32)

    def tiles(n):
        return jax.ShapeDtypeStruct((2, n, 8, 128), f32)

    def buf(n):
        return pltpu.VMEM((2, n, 32, 256), f32)

    def call(body, ins, outs, scratch, flops, mib, aliases=None):
        return pl.pallas_call(
            body,
            in_specs=ins,
            out_specs=[s for s, _ in outs],
            out_shape=[a for _, a in outs],
            scratch_shapes=scratch,
            input_output_aliases=aliases or {},
            compiler_params=pltpu.CompilerParams(vmem_limit_bytes=mib << 20),
            cost_estimate=pl.CostEstimate(flops=flops, bytes_accessed=1 << 20, transcendentals=0),
            name=body.__name__,
        )

    count = lax.axis_size("gz")
    across = [(i, i if i in (0, count - 1) else i + 1 if i % 2 else i - 1) for i in range(count)]
    within = [(i, i ^ 1) for i in range(count)]

    outer, own5, inner, d1, d2, d3, d4, d5, s5 = call(
        transform,
        [hbm],
        [(vmem, arr(n)) for n in (FAR, 2, ALL, 32, 16, 8, 4, 2, 2)],
        [buf(64), pltpu.SemaphoreType.DMA((8,))],
        20_000_000,
        TRANSFORM_MIB,
    )(fields)
    outer = lax.ppermute(outer, "gz", across)
    inner = lax.ppermute(inner, "gz", within)
    (own5,) = call(hand_on, [vmem] * 2, [(vmem, arr(2))], [], 5_000_000, 4)(own5, inner)
    outer5 = lax.ppermute(own5, "gz", across)
    o1, o2, o3, sums_a = call(
        interiors,
        [smem] + [vmem] * 4,
        [(hbm, arr(32)), (hbm, arr(16)), (hbm, arr(8)), (vmem, tiles(3))],
        [buf(32), buf(16), buf(8), pltpu.SemaphoreType.DMA((6,))],
        2_000_000_000,
        8,
    )(threshold, d1, d2, d3, own5)
    (relayed,) = call(hand_in, [vmem] * 2, [(vmem, arr(2))], [], 5_000_000, 4)(outer, sums_a)
    received = lax.ppermute(relayed, "gz", within)
    b1, b2, b3, b4, base, ends, sums_b = call(
        edges,
        [smem] + [vmem] * 9,
        [(vmem, arr(n)) for n in (3, 5, 6, 4, 4, 2)] + [(vmem, tiles(4))],
        [],
        1_000_000_000,
        4,
    )(threshold, outer, inner, d1, d2, d3, d4, d5, s5, relayed)
    b5, b6, total = call(
        fifth,
        [smem] + [vmem] * 7,
        [(vmem, arr(2)), (vmem, arr(2)), (vmem, jax.ShapeDtypeStruct((1, 128), f32))],
        [pltpu.VMEM((2, 2, 8, 128), f32)],
        5_000_000,
        4,
    )(threshold, outer5, inner, received, base, ends, sums_a, sums_b)

    devices = count * lax.axis_size("xy")
    parts = lax.all_to_all(jnp.broadcast_to(total, (devices, 1, 128)), ("gz", "xy"), 0, 0, tiled=True)
    cells = np.zeros((1, 128), np.float32) + 1.0
    cells[0, :12] = [n * 32 * 256 * devices for n in (32, 16, 8, 4, 2, 2)] * 2
    o1, o2, o3, o4, o5, o6, energy = call(
        finish,
        [vmem] * 8 + [hbm] * 3,
        [(hbm, arr(n)) for n in (32, 16, 8, 4, 2, 2)] + [(vmem, jax.ShapeDtypeStruct((2, 6), f32))],
        [pltpu.SemaphoreType.DMA((15,))],
        5_000_000,
        4,
        {8: 0, 9: 1, 10: 2},
    )(cells, parts, b1, b2, b3, b4, b5, b6, o1, o2, o3)
    return o1, o2, o3, o4, o5, o6, energy


def solution(mesh):
    split = P(None, "gz", "xy", None)
    return jax.shard_map(local, mesh=mesh, in_specs=(split, P()), out_specs=(split,) * 6 + (P(),), check_vma=False)
```

```python
import functools

import jax
import jax.numpy as jnp
import numpy as np
from jax import lax
from jax.experimental import pallas as pl
from jax.experimental.pallas import tpu as pltpu
from jax.sharding import PartitionSpec as P


ALPHA = -1.586134342059924
BETA = -0.052980118572961
GAMMA = 0.882911075530934
DELTA = 0.443506852043971
KAPPA = 1.230174104914001
SQRT_TWO = 1.4142135623730951
LOW = SQRT_TWO / KAPPA
HIGH = KAPPA / SQRT_TWO
LEVELS = 5
FAR = 8
ALL = 2 * LEVELS
EDGE_LO = (1, 2, 3)
EDGE_HI = (2, 3, 3)


class Level:
    def __init__(self, n, left, right, emit_d, emit_s):
        self.n, self.left, self.right, self.emit_d, self.emit_s = n, left, right, emit_d, emit_s
        self.s, self.d, self.d1, self.s2, self.d3 = [], [], [], [], []

    def push(self, x):
        if len(self.s) == len(self.d):
            self.s.append(x)
            i = len(self.s) - 2
            if i >= 0:
                self.add(self.d[i] + ALPHA * (self.s[i] + self.s[i + 1]))
        else:
            self.d.append(x)
            if len(self.d) == self.n:
                self.finish()

    def add(self, v):
        self.d1.append(v)
        i = len(self.d1) - 1
        if i == 0:
            self.p = ALPHA * self.s[0]
            self.c = self.s[0] + BETA * v
            return
        if i == 1:
            a, b = self.left(self)
            below = a + self.p
            self.s2.append(self.c + BETA * below)
            self.d3m = below + GAMMA * ((b + BETA * below) + self.s2[0])
        if i == self.n - 1:
            self.s2.append(self.b + BETA * v)
        else:
            self.s2.append(self.s[i] + BETA * (self.d1[i - 1] + v))
        self.third(i - 1, self.s2[i])

    def third(self, j, above):
        self.d3.append(self.d1[j] + GAMMA * (self.s2[j] + above))
        self.emit_d(j, self.d3[j])
        before = self.d3[j - 1] if j else self.d3m
        self.emit_s(j, self.s2[j] + DELTA * (before + self.d3[j]))

    def finish(self):
        n = self.n
        self.a = self.d[n - 1] + ALPHA * self.s[n - 1]
        self.b = self.s[n - 1] + BETA * self.d1[n - 2]
        p, c = self.right(self)
        v = self.a + p
        self.add(v)
        self.third(n - 1, c + BETA * v)


def low_end(level):
    return level.d[0] + ALPHA * level.s[1], level.s[1] + BETA * level.d1[1]


def high_end(level):
    return ALPHA * level.s[-1], level.b


@functools.cache
def response(side, length=1024):
    zero, unit = np.zeros(2 * LEVELS), np.eye(2 * LEVELS)
    found, u = [], [zero] * length
    for l in range(LEVELS):
        n = len(u) // 2
        state, none = (unit[2 * l], unit[2 * l + 1]), (zero, zero)
        d, s = [None] * n, [None] * n
        level = Level(
            n,
            lambda _: state if side == "lo" else none,
            lambda _: state if side == "hi" else none,
            d.__setitem__,
            s.__setitem__,
        )
        for x in u:
            level.push(x)
        u = s
        down, up = (level.p, level.c), (level.a, level.b)
        found.append((down, up, d, s) if side == "lo" else (up, down, d[::-1], s[::-1]))
    return found


TRANSFORM_MIB = 47
BACK, ON, DETAIL, APPROX = range(4)


def combine(row, states):
    total = None
    for k, x in zip(row, states):
        if k != 0.0:
            term = float(k) * x
            total = term if total is None else total + term
    return total


def where_am_i():
    z = lax.axis_index("gz")
    return lax.rem(z, 2) == 1, z == 0, z == lax.axis_size("gz") - 1


def over_tiles(body, fields=(0, 1), unroll=2):
    for f in fields:

        def step(i, carry, f=f):
            rows = pl.ds(pl.multiple_of((i // 2) * 8, 8), 8)
            body(f, rows, pl.ds(pl.multiple_of(lax.rem(i, 2) * 128, 128), 128))
            return carry

        lax.fori_loop(0, 8, step, 0, unroll=unroll)


def transform(x_hbm, outer, outer5, inner, d1, d2, d3, d4, d5, s5, x_vmem, sem):
    upper, lowest, highest = where_am_i()

    def fetch(j):
        rows = pl.ds(pl.multiple_of(lax.rem(j, 4) * 8, 8), 8)
        at = (j // 4, slice(None), rows)
        return pltpu.make_async_copy(x_hbm.at[at], x_vmem.at[at], sem.at[j])

    for j in range(8):
        fetch(j).start()
    bands = (d1, d2, d3, d4, d5)
    from_above, from_below = response("hi"), response("lo")

    def tile(i, carry):
        @pl.when(lax.rem(i, 2) == 0)
        def _():
            fetch(i // 2).wait()

        f = i // 8
        rows = pl.ds(pl.multiple_of(lax.rem(i // 2, 4) * 8, 8), 8)
        cols = pl.ds(pl.multiple_of(lax.rem(i, 2) * 128, 128), 128)
        down, up, levels = [], [], []

        def left(l):
            def state(level):
                down.extend((level.p, level.c))
                end = low_end(level)
                if l == 0:
                    return tuple(jnp.where(lowest, e, 0.0) for e in end)
                return tuple(jnp.where(lowest, e, combine(r, down)) for e, r in zip(end, from_above[l][BACK]))

            return state

        def right(l):
            def state(level):
                up.extend((level.a, level.b))
                end = high_end(level)
                if l == 0:
                    return tuple(jnp.where(highest, e, 0.0) for e in end)
                return tuple(jnp.where(highest, e, combine(r, up)) for e, r in zip(end, from_below[l][BACK]))

            return state

        def keep(l):
            def store(j, v):
                bands[l][f, j, rows, cols] = v

            return store

        def pass_on(l):
            def store(j, v):
                if l == LEVELS - 1:
                    s5[f, j, rows, cols] = v
                else:
                    levels[l + 1].push(v)

            return store

        for l in range(LEVELS):
            levels.append(Level(32 >> l, left(l), right(l), keep(l), pass_on(l)))
        for z in range(64):
            levels[0].push(x_vmem[f, z, rows, cols])
        for k in range(ALL):
            out = jnp.where(upper, up[k], down[k])
            if k < FAR:
                outer[f, k, rows, cols] = out
            else:
                outer5[f, k - FAR, rows, cols] = out
            inner[f, k, rows, cols] = jnp.where(upper, down[k], up[k])
        return carry

    lax.fori_loop(0, 16, tile, 0)


def shrink(v, scale, limit):
    v = v * scale
    return v - jnp.clip(v, -limit, limit)


def corrected(v, *parts):
    for row, states in parts:
        term = combine(row, states)
        if term is not None:
            v = term if v is None else v + term
    return v


def through(states, upper):
    lo, hi = response("lo", 64)[4][ON], response("hi", 64)[4][ON]
    sums = []
    for k in range(2):
        row = [jnp.where(upper, float(x), float(y)) for x, y in zip(lo[k], hi[k])]
        total = row[0] * states[0]
        for x, state in list(zip(row, states))[1:]:
            total = total + x * state
        sums.append(total)
    return sums


def hand_on(own5, inner, out5):
    upper, _, _ = where_am_i()

    def tile(f, rows, cols):
        extra = through([inner[f, k, rows, cols] for k in range(FAR)], upper)
        for k in range(2):
            out5[f, k, rows, cols] = own5[f, k, rows, cols] + extra[k]

    over_tiles(tile)


def hand_in(outer, after, out5):
    upper, lowest, highest = where_am_i()
    end = jnp.logical_or(lowest, highest)

    def tile(f, rows, cols):
        extra = through([outer[f, k, rows, cols] for k in range(FAR)], jnp.logical_not(upper))
        for k in range(2):
            out5[f, k, rows, cols] = jnp.where(end, 0.0, extra[k])

    over_tiles(tile)


def add_parts(lo, hi, upper_side, states, v4, v5, v6, f, rows, cols, out4, out5, out6):
    rows_of = hi if upper_side else lo
    for src, dst, l, kind, n in ((v4, out4, 3, DETAIL, 4), (v5, out5, 4, DETAIL, 2), (v6, out6, 4, APPROX, 2)):
        for j in range(n):
            row = rows_of[l][kind][n - 1 - j if upper_side else j][:FAR]
            dst[f, j, rows, cols] = corrected(src[f, j, rows, cols], (row, states))


def side(upper_side, l):
    return ((32 >> l) - EDGE_HI[l], EDGE_HI[l]) if upper_side else (0, EDGE_LO[l])


def near(limits, d1, d2, d3, d4, d5, s5, inner, after, o1, o2, o3, n4, n5, n6, ends, sums, b1, b2, b3, acc, sem):
    upper, lowest, highest = where_am_i()
    lo, hi = response("lo"), response("hi")
    pass_up = response("lo", 64)[4][ON]
    triples = ((d1, b1, o1), (d2, b2, o2), (d3, b3, o3))
    copies = []
    for f in range(2):
        limit = limits[f]
        for l, (raw, buf, out) in enumerate(triples):
            first, last = EDGE_LO[l], (32 >> l) - EDGE_HI[l]

            def layer(z, total, raw=raw, buf=buf, l=l):
                v = shrink(raw[f, z], LOW**l * HIGH, limit)
                buf[f, z] = v
                return total + v * v

            total = lax.fori_loop(first, last, layer, jnp.zeros((32, 256), jnp.float32), unroll=True)
            total = total.reshape(4, 8, 256).sum(axis=0)
            acc[f, l] = total[:, :128] + total[:, 128:]
            at = (f, pl.ds(first, last - first))
            copy = pltpu.make_async_copy(buf.at[at], out.at[at], sem.at[3 * f + l])
            copy.start()
            copies.append(copy)

    def inner_side(upper_side):
        def tile(f, rows, cols):
            limit = limits[f]
            states = [inner[f, k, rows, cols] for k in range(FAR)]
            for l, (raw, buf, _) in enumerate(triples):
                start, size = side(upper_side, l)
                total = acc[f, l]
                for j in range(start, start + size):
                    row = hi[l][DETAIL][(32 >> l) - 1 - j] if upper_side else lo[l][DETAIL][j]
                    v = shrink(corrected(raw[f, j, rows, cols], (row, states)), LOW**l * HIGH, limit)
                    buf[f, j, rows, cols] = v
                    total = total + v * v
                acc[f, l] = total
            add_parts(lo, hi, upper_side, states, d4, d5, s5, f, rows, cols, n4, n5, n6)

        over_tiles(tile)
        pieces = []
        for f in range(2):
            for l, (_, buf, out) in enumerate(triples):
                at = (f, pl.ds(*side(upper_side, l)))
                pieces.append(pltpu.make_async_copy(buf.at[at], out.at[at], sem.at[6 + 3 * f + l]))
        for piece in pieces:
            piece.start()
        for piece in pieces:
            piece.wait()

    @pl.when(jnp.logical_not(jnp.logical_or(lowest, highest)))
    def _():
        ends[...] = jnp.zeros(ends.shape, jnp.float32)

    @pl.when(lowest)
    def _():
        def tile(f, rows, cols):
            above = [inner[f, k, rows, cols] for k in range(FAR)]
            u = [combine(hi[3][APPROX][3 - j], above) for j in range(4)]
            ends[f, 0, rows, cols] = u[1] + ALPHA * u[2]
            ends[f, 1, rows, cols] = u[2] + BETA * ((u[3] + ALPHA * u[2]) + inner[f, FAR, rows, cols])

        over_tiles(tile)

    @pl.when(highest)
    def _():
        def tile(f, rows, cols):
            below = [inner[f, k, rows, cols] for k in range(FAR)]
            ends[f, 0, rows, cols] = ALPHA * combine(lo[3][APPROX][2], below)
            ends[f, 1, rows, cols] = combine(pass_up[1], below)

        over_tiles(tile)

    @pl.when(upper)
    def _():
        inner_side(False)

    @pl.when(jnp.logical_not(upper))
    def _():
        inner_side(True)

    sums[...] = acc[...]
    for copy in copies:
        copy.wait()


def edges(limits, outer, d1, d2, d3, n4, n5, n6, after, b1, b2, b3, b4, m5, m6, sums):
    upper, lowest, highest = where_am_i()
    end = jnp.logical_or(lowest, highest)
    lo, hi = response("lo"), response("hi")
    sums[...] = jnp.zeros(sums.shape, jnp.float32)

    def outer_side(upper_side):
        def tile(f, rows, cols):
            limit = limits[f]
            states = [jnp.where(end, 0.0, outer[f, k, rows, cols]) for k in range(FAR)]
            for l, (raw, buf) in enumerate(((d1, b1), (d2, b2), (d3, b3))):
                start, size = side(upper_side, l)
                total = sums[f, l]
                for k in range(size):
                    j = start + k
                    row = hi[l][DETAIL][(32 >> l) - 1 - j] if upper_side else lo[l][DETAIL][j]
                    v = shrink(corrected(raw[f, j, rows, cols], (row, states)), LOW**l * HIGH, limit)
                    buf[f, k, rows, cols] = v
                    total = total + v * v
                sums[f, l] = total
            add_parts(lo, hi, upper_side, states, n4, n5, n6, f, rows, cols, b4, m5, m6)
            total = sums[f, 3]
            for j in range(4):
                v = shrink(b4[f, j, rows, cols], LOW**3 * HIGH, limit)
                b4[f, j, rows, cols] = v
                total = total + v * v
            sums[f, 3] = total

        over_tiles(tile)

    @pl.when(upper)
    def _():
        outer_side(True)

    @pl.when(jnp.logical_not(upper))
    def _():
        outer_side(False)


def fifth(limits, outer5, inner, relayed, m5, m6, ends, sums_a, sums_b, b5, b6, total, acc):
    upper, lowest, highest = where_am_i()
    lo, hi = response("lo")[4], response("hi")[4]
    acc[...] = jnp.zeros(acc.shape, jnp.float32)

    def tile(f, rows, cols):
        limit = limits[f]
        below, above = [], []
        for k in range(2):
            o = outer5[f, k, rows, cols]
            n = inner[f, FAR + k, rows, cols] + relayed[f, k, rows, cols]
            e = ends[f, k, rows, cols]
            below.append(jnp.where(lowest, e, jnp.where(upper, n, o)))
            above.append(jnp.where(highest, e, jnp.where(upper, o, n)))
        for j in range(2):
            d = corrected(m5[f, j, rows, cols], (lo[DETAIL][j][FAR:], below), (hi[DETAIL][1 - j][FAR:], above))
            d = shrink(d, LOW**4 * HIGH, limit)
            b5[f, j, rows, cols] = d
            s = corrected(m6[f, j, rows, cols], (lo[APPROX][j][FAR:], below), (hi[APPROX][1 - j][FAR:], above))
            s = shrink(s, LOW**5, limit)
            b6[f, j, rows, cols] = s
            acc[f, 0] += d * d
            acc[f, 1] += s * s

    over_tiles(tile)
    lane = lax.broadcasted_iota(jnp.int32, (1, 128), 1)
    row = jnp.zeros((1, 128), jnp.float32)
    for f in range(2):
        for b in range(6):
            if b < 3:
                part = sums_a[f, b] + sums_b[f, b]
            elif b < 4:
                part = sums_b[f, b]
            else:
                part = acc[f, b - 4]
            row = row + jnp.where(lane == 6 * f + b, jnp.sum(part), 0.0)
    total[...] = row


def finish(cells, parts, b1, b2, b3, b4, b5, b6, o1_in, o2_in, o3_in, o1, o2, o3, o4, o5, o6, energy, row_vmem, sem):
    upper, _, _ = where_am_i()
    copies = [pltpu.make_async_copy(a, b, sem.at[k]) for k, (a, b) in enumerate(((b4, o4), (b5, o5), (b6, o6)))]
    for copy in copies:
        copy.start()

    def outer_side(upper_side):
        for f in range(2):
            for l, (buf, out) in enumerate(((b1, o1), (b2, o2), (b3, o3))):
                start, size = side(upper_side, l)
                yield pltpu.make_async_copy(
                    buf.at[f, pl.ds(0, size)], out.at[f, pl.ds(start, size)], sem.at[4 + 3 * f + l]
                )

    @pl.when(upper)
    def _():
        for copy in outer_side(True):
            copy.start()

    @pl.when(jnp.logical_not(upper))
    def _():
        for copy in outer_side(False):
            copy.start()

    row = jnp.sum(parts[...], axis=0) * (1.0 / cells[...])
    row_vmem[0:1, :] = row[:, 0:6]
    row_vmem[1:2, :] = row[:, 6:12]
    copies.append(pltpu.make_async_copy(row_vmem, energy, sem.at[3]))
    copies[-1].start()
    for copy in copies:
        copy.wait()

    @pl.when(upper)
    def _():
        for copy in outer_side(True):
            copy.wait()

    @pl.when(jnp.logical_not(upper))
    def _():
        for copy in outer_side(False):
            copy.wait()


def local(fields, threshold):
    f32 = jnp.float32
    vmem, hbm, smem = (pl.BlockSpec(memory_space=m) for m in (pltpu.VMEM, pltpu.HBM, pltpu.SMEM))

    def arr(n):
        return jax.ShapeDtypeStruct((2, n, 32, 256), f32)

    def tiles(n):
        return jax.ShapeDtypeStruct((2, n, 8, 128), f32)

    def buf(n):
        return pltpu.VMEM((2, n, 32, 256), f32)

    def call(body, ins, outs, scratch, flops, mib, aliases=None):
        return pl.pallas_call(
            body,
            in_specs=ins,
            out_specs=[s for s, _ in outs],
            out_shape=[a for _, a in outs],
            scratch_shapes=scratch,
            input_output_aliases=aliases or {},
            compiler_params=pltpu.CompilerParams(vmem_limit_bytes=mib << 20),
            cost_estimate=pl.CostEstimate(flops=flops, bytes_accessed=1 << 20, transcendentals=0),
        )

    count = lax.axis_size("gz")
    across = [(i, (i + 1) % count if i % 2 else (i - 1) % count) for i in range(count)]
    within = [(i, i ^ 1) for i in range(count)]

    outer, own5, inner, d1, d2, d3, d4, d5, s5 = call(
        transform,
        [hbm],
        [(vmem, arr(n)) for n in (FAR, 2, ALL, 32, 16, 8, 4, 2, 2)],
        [buf(64), pltpu.SemaphoreType.DMA((8,))],
        20_000_000,
        TRANSFORM_MIB,
    )(fields)
    outer = lax.ppermute(outer, "gz", across)
    inner = lax.ppermute(inner, "gz", within)
    (own5,) = call(hand_on, [vmem] * 2, [(vmem, arr(2))], [], 5_000_000, 4)(own5, inner)
    outer5 = lax.ppermute(own5, "gz", across)
    o1, o2, o3, n4, n5, n6, ends, sums_a = call(
        near,
        [smem] + [vmem] * 8,
        [(hbm, arr(32)), (hbm, arr(16)), (hbm, arr(8))] + [(vmem, arr(n)) for n in (4, 2, 2, 2)] + [(vmem, tiles(3))],
        [buf(32), buf(16), buf(8), pltpu.VMEM((2, 3, 8, 128), f32), pltpu.SemaphoreType.DMA((12,))],
        2_000_000_000,
        8,
    )(threshold, d1, d2, d3, d4, d5, s5, inner, own5)
    (relayed,) = call(hand_in, [vmem] * 2, [(vmem, arr(2))], [], 5_000_000, 4)(outer, sums_a)
    received = lax.ppermute(relayed, "gz", within)
    b1, b2, b3, b4, m5, m6, sums_b = call(
        edges,
        [smem] + [vmem] * 8,
        [(vmem, arr(n)) for n in (2, 3, 3, 4, 2, 2)] + [(vmem, tiles(4))],
        [],
        1_000_000_000,
        4,
    )(threshold, outer, d1, d2, d3, n4, n5, n6, relayed)
    b5, b6, total = call(
        fifth,
        [smem] + [vmem] * 8,
        [(vmem, arr(2)), (vmem, arr(2)), (vmem, jax.ShapeDtypeStruct((1, 128), f32))],
        [pltpu.VMEM((2, 2, 8, 128), f32)],
        5_000_000,
        4,
    )(threshold, outer5, inner, received, m5, m6, ends, sums_a, sums_b)

    devices = count * lax.axis_size("xy")
    parts = lax.all_to_all(jnp.broadcast_to(total, (devices, 1, 128)), ("gz", "xy"), 0, 0, tiled=True)
    cells = np.zeros((1, 128), np.float32) + 1.0
    cells[0, :12] = [n * 32 * 256 * devices for n in (32, 16, 8, 4, 2, 2)] * 2
    o1, o2, o3, o4, o5, o6, energy = call(
        finish,
        [vmem] * 8 + [hbm] * 3,
        [(hbm, arr(n)) for n in (32, 16, 8, 4, 2, 2)] + [(hbm, jax.ShapeDtypeStruct((2, 6), f32))],
        [pltpu.VMEM((2, 6), f32), pltpu.SemaphoreType.DMA((10,))],
        5_000_000,
        4,
        {8: 0, 9: 1, 10: 2},
    )(cells, parts, b1, b2, b3, b4, b5, b6, o1, o2, o3)
    return o1, o2, o3, o4, o5, o6, energy


def solution(mesh):
    split = P(None, "gz", "xy", None)

    def step(fields, threshold):
        return local(fields, threshold)

    step = jax.shard_map(step, mesh=mesh, in_specs=(split, P()), out_specs=(split,) * 6 + (P(),), check_vma=False)
    return step
```

```python
import functools

import jax
import jax.numpy as jnp
import numpy as np
from jax import lax
from jax.experimental import pallas as pl
from jax.experimental.pallas import tpu as pltpu
from jax.sharding import PartitionSpec as P


ALPHA = -1.586134342059924
BETA = -0.052980118572961
GAMMA = 0.882911075530934
DELTA = 0.443506852043971
KAPPA = 1.230174104914001
SQRT_TWO = 1.4142135623730951
LOW = SQRT_TWO / KAPPA
HIGH = KAPPA / SQRT_TWO
LEVELS = 5
FAR = 8
ALL = 2 * LEVELS
EDGE_LO = (1, 2, 3)
EDGE_HI = (2, 3, 3)


class Level:
    def __init__(self, n, left, right, emit_d, emit_s):
        self.n, self.left, self.right, self.emit_d, self.emit_s = n, left, right, emit_d, emit_s
        self.s, self.d, self.d1, self.s2, self.d3 = [], [], [], [], []

    def push(self, x):
        if len(self.s) == len(self.d):
            self.s.append(x)
            i = len(self.s) - 2
            if i >= 0:
                self.add(self.d[i] + ALPHA * (self.s[i] + self.s[i + 1]))
        else:
            self.d.append(x)
            if len(self.d) == self.n:
                self.finish()

    def add(self, v):
        self.d1.append(v)
        i = len(self.d1) - 1
        if i == 0:
            self.p = ALPHA * self.s[0]
            self.c = self.s[0] + BETA * v
            return
        if i == 1:
            a, b = self.left(self)
            below = a + self.p
            self.s2.append(self.c + BETA * below)
            self.d3m = below + GAMMA * ((b + BETA * below) + self.s2[0])
        if i == self.n - 1:
            self.s2.append(self.b + BETA * v)
        else:
            self.s2.append(self.s[i] + BETA * (self.d1[i - 1] + v))
        self.third(i - 1, self.s2[i])

    def third(self, j, above):
        self.d3.append(self.d1[j] + GAMMA * (self.s2[j] + above))
        self.emit_d(j, self.d3[j])
        before = self.d3[j - 1] if j else self.d3m
        self.emit_s(j, self.s2[j] + DELTA * (before + self.d3[j]))

    def finish(self):
        n = self.n
        self.a = self.d[n - 1] + ALPHA * self.s[n - 1]
        self.b = self.s[n - 1] + BETA * self.d1[n - 2]
        p, c = self.right(self)
        v = self.a + p
        self.add(v)
        self.third(n - 1, c + BETA * v)


def low_end(level):
    return level.d[0] + ALPHA * level.s[1], level.s[1] + BETA * level.d1[1]


def high_end(level):
    return ALPHA * level.s[-1], level.b


@functools.cache
def response(side, length=1024):
    zero, unit = np.zeros(2 * LEVELS), np.eye(2 * LEVELS)
    found, u = [], [zero] * length
    for l in range(LEVELS):
        n = len(u) // 2
        state, none = (unit[2 * l], unit[2 * l + 1]), (zero, zero)
        d, s = [None] * n, [None] * n
        level = Level(
            n,
            lambda _: state if side == "lo" else none,
            lambda _: state if side == "hi" else none,
            d.__setitem__,
            s.__setitem__,
        )
        for x in u:
            level.push(x)
        u = s
        down, up = (level.p, level.c), (level.a, level.b)
        found.append((down, up, d, s) if side == "lo" else (up, down, d[::-1], s[::-1]))
    return found


TRANSFORM_MIB = 46
BACK, ON, DETAIL, APPROX = range(4)


def combine(row, states):
    total = None
    for k, x in zip(row, states):
        if k != 0.0:
            term = float(k) * x
            total = term if total is None else total + term
    return total


def where_am_i():
    z = lax.axis_index("gz")
    return lax.rem(z, 2) == 1, z == 0, z == lax.axis_size("gz") - 1


def over_tiles(body, fields=(0, 1)):
    for f in fields:
        for rows in range(0, 32, 8):
            for cols in range(0, 256, 128):
                body(f, pl.ds(rows, 8), pl.ds(cols, 128))


class Sums:
    def __init__(self):
        self.parts = {}

    def add(self, key, v):
        self.parts[key] = self.parts[key] + v * v if key in self.parts else v * v


def first_half(x_hbm, outer, own5, passed, inner, d1, d2, d3, d4, d5, s5, x_next, x_vmem, sem):
    copies = []
    for j in range(4):
        rows = pl.ds(8 * j, 8)
        copies.append(pltpu.make_async_copy(x_hbm.at[0, :, rows], x_vmem.at[:, rows], sem.at[j]))
    copies.append(pltpu.make_async_copy(x_hbm.at[1], x_next, sem.at[4]))
    for copy in copies:
        copy.start()

    def fetched(j):
        rows = pl.ds(pl.multiple_of(8 * j, 8), 8)
        pltpu.make_async_copy(x_hbm.at[0, :, rows], x_vmem.at[:, rows], sem.at[j]).wait()

    transform(x_vmem, outer, own5, passed, inner, (d1, d2, d3, d4, d5), s5, 0, fetched)
    copies[4].wait()


def second_half(*refs):
    outer, own5, passed, inner, d1, d2, d3, d4, d5, s5 = refs[-10:]
    transform(refs[0], outer, own5, passed, inner, (d1, d2, d3, d4, d5), s5, 1, None)


def transform(x, outer, outer5, passed, inner, bands, s5, f, fetched):
    upper, lowest, highest = where_am_i()
    from_above, from_below = response("hi"), response("lo")

    def tile(i, carry):
        if fetched is not None:

            @pl.when(lax.rem(i, 2) == 0)
            def _():
                fetched(i // 2)

        rows = pl.ds(pl.multiple_of((i // 2) * 8, 8), 8)
        cols = pl.ds(pl.multiple_of(lax.rem(i, 2) * 128, 128), 128)
        down, up, levels = [], [], []

        def left(l):
            def state(level):
                down.extend((level.p, level.c))
                end = low_end(level)
                if l == 0:
                    return tuple(jnp.where(lowest, e, 0.0) for e in end)
                return tuple(jnp.where(lowest, e, combine(r, down)) for e, r in zip(end, from_above[l][BACK]))

            return state

        def right(l):
            def state(level):
                up.extend((level.a, level.b))
                end = high_end(level)
                if l == 0:
                    return tuple(jnp.where(highest, e, 0.0) for e in end)
                return tuple(jnp.where(highest, e, combine(r, up)) for e, r in zip(end, from_below[l][BACK]))

            return state

        def keep(l):
            def store(j, v):
                bands[l][f, j, rows, cols] = v

            return store

        def pass_on(l):
            def store(j, v):
                if l == LEVELS - 1:
                    s5[f, j, rows, cols] = v
                else:
                    levels[l + 1].push(v)

            return store

        for l in range(LEVELS):
            levels.append(Level(32 >> l, left(l), right(l), keep(l), pass_on(l)))
        for z in range(64):
            levels[0].push(x[z, rows, cols])
        for k in range(ALL):
            out = jnp.where(upper, up[k], down[k])
            if k < FAR:
                outer[k, rows, cols] = out
            else:
                outer5[f, k - FAR, rows, cols] = out
        inwards = [jnp.where(upper, y, x) for x, y in zip(up, down)]
        for k in range(ALL):
            inner[f, k, rows, cols] = inwards[k]
        for k, v in enumerate(through(inwards[:FAR], jnp.logical_not(upper))):
            passed[f, k, rows, cols] = v
        return carry

    lax.fori_loop(0, 8, tile, 0)


def shrink(v, scale, limit):
    v = v * scale
    return v - jnp.clip(v, -limit, limit)


def corrected(v, *parts):
    for row, states in parts:
        term = combine(row, states)
        if term is not None:
            v = term if v is None else v + term
    return v


def through(states, upper):
    lo, hi = response("lo", 64)[4][ON], response("hi", 64)[4][ON]
    sums = []
    for k in range(2):
        row = [jnp.where(upper, float(x), float(y)) for x, y in zip(lo[k], hi[k])]
        total = row[0] * states[0]
        for x, state in list(zip(row, states))[1:]:
            total = total + x * state
        sums.append(total)
    return sums


def hand_on(own5, passed, out5):
    out5[...] = own5[...] + passed[...]


def hand_in(outer_a, outer_b, after, out5):
    upper, lowest, highest = where_am_i()
    end = jnp.logical_or(lowest, highest)

    def tile(f, rows, cols):
        extra = through([(outer_a, outer_b)[f][k, rows, cols] for k in range(FAR)], jnp.logical_not(upper))
        for k in range(2):
            out5[f, k, rows, cols] = jnp.where(end, 0.0, extra[k])

    over_tiles(tile)


def add_parts(lo, hi, upper_side, states, v4, v5, v6, f, rows, cols):
    rows_of, sums = (hi if upper_side else lo), {}
    for i, (src, l, kind, n) in enumerate(((v4, 3, DETAIL, 4), (v5, 4, DETAIL, 2), (v6, 4, APPROX, 2))):
        for j in range(n):
            row = rows_of[l][kind][n - 1 - j if upper_side else j][:FAR]
            sums[i, j] = corrected(src[f, j, rows, cols], (row, states))
    return sums


def side(upper_side, l):
    return ((32 >> l) - EDGE_HI[l], EDGE_HI[l]) if upper_side else (0, EDGE_LO[l])


def interiors(limits, d1, d2, d3, b1, b2, b3, sums):
    for f in range(2):
        limit = limits[f]
        for l, (raw, buf) in enumerate(((d1, b1), (d2, b2), (d3, b3))):

            def layer(z, total, raw=raw, buf=buf, l=l):
                v = shrink(raw[f, z], LOW**l * HIGH, limit)
                buf[f, z] = v
                return total + v * v

            zero = jnp.zeros((32, 256), jnp.float32)
            total = lax.fori_loop(EDGE_LO[l], (32 >> l) - EDGE_HI[l], layer, zero, unroll=True)
            total = total.reshape(4, 8, 256).sum(axis=0)
            sums[f, l] = total[:, :128] + total[:, 128:]


def near(limits, d1, d2, d3, d4, d5, s5, inner, after, c1, c2, c3, acc, o1, o2, o3, n4, n5, n6, ends, sums, e1, e2, e3, sem):
    upper, lowest, highest = where_am_i()
    lo, hi = response("lo"), response("hi")
    pass_up = response("lo", 64)[4][ON]
    triples = ((d1, e1, o1), (d2, e2, o2), (d3, e3, o3))
    copies = []
    for f in range(2):
        for l, (buf, out) in enumerate(((c1, o1), (c2, o2), (c3, o3))):
            first, last = EDGE_LO[l], (32 >> l) - EDGE_HI[l]
            at = (f, pl.ds(first, last - first))
            copies.append(pltpu.make_async_copy(buf.at[at], out.at[at], sem.at[3 * f + l]))
    for copy in copies:
        copy.start()

    def inner_side(upper_side):
        found = Sums()

        def tile(f, rows, cols):
            limit = limits[f]
            states = [inner[f, k, rows, cols] for k in range(FAR)]
            for l, (raw, buf, _) in enumerate(triples):
                start, size = side(upper_side, l)
                for k in range(size):
                    j = start + k
                    row = hi[l][DETAIL][(32 >> l) - 1 - j] if upper_side else lo[l][DETAIL][j]
                    v = shrink(corrected(raw[f, j, rows, cols], (row, states)), LOW**l * HIGH, limit)
                    buf[f, k, rows, cols] = v
                    found.add((f, l), v)
            for (l, j), v in add_parts(lo, hi, upper_side, states, d4, d5, s5, f, rows, cols).items():
                (n4, n5, n6)[l][f, j, rows, cols] = v

        over_tiles(tile)
        for (f, l), part in found.parts.items():
            sums[f, l] = acc[f, l] + part
        pieces = []
        for f in range(2):
            for l, (_, buf, out) in enumerate(triples):
                start, size = side(upper_side, l)
                pieces.append(
                    pltpu.make_async_copy(
                        buf.at[f, pl.ds(0, size)], out.at[f, pl.ds(start, size)], sem.at[6 + 3 * f + l]
                    )
                )
        for piece in pieces:
            piece.start()
        for piece in pieces:
            piece.wait()

    @pl.when(jnp.logical_not(jnp.logical_or(lowest, highest)))
    def _():
        ends[...] = jnp.zeros(ends.shape, jnp.float32)

    @pl.when(lowest)
    def _():
        def tile(f, rows, cols):
            above = [inner[f, k, rows, cols] for k in range(FAR)]
            u = [combine(hi[3][APPROX][3 - j], above) for j in range(4)]
            ends[f, 0, rows, cols] = u[1] + ALPHA * u[2]
            ends[f, 1, rows, cols] = u[2] + BETA * ((u[3] + ALPHA * u[2]) + inner[f, FAR, rows, cols])

        over_tiles(tile)

    @pl.when(highest)
    def _():
        def tile(f, rows, cols):
            below = [inner[f, k, rows, cols] for k in range(FAR)]
            ends[f, 0, rows, cols] = ALPHA * combine(lo[3][APPROX][2], below)
            ends[f, 1, rows, cols] = combine(pass_up[1], below)

        over_tiles(tile)

    @pl.when(upper)
    def _():
        inner_side(False)

    @pl.when(jnp.logical_not(upper))
    def _():
        inner_side(True)

    for copy in copies:
        copy.wait()


def edges(limits, outer_a, outer_b, d1, d2, d3, n4, n5, n6, after, b1, b2, b3, b4, m5, m6, sums):
    upper, lowest, highest = where_am_i()
    end = jnp.logical_or(lowest, highest)
    lo, hi = response("lo"), response("hi")

    def outer_side(upper_side):
        found = Sums()

        def tile(f, rows, cols):
            limit = limits[f]
            states = [jnp.where(end, 0.0, (outer_a, outer_b)[f][k, rows, cols]) for k in range(FAR)]
            for l, (raw, buf) in enumerate(((d1, b1), (d2, b2), (d3, b3))):
                start, size = side(upper_side, l)
                for k in range(size):
                    j = start + k
                    row = hi[l][DETAIL][(32 >> l) - 1 - j] if upper_side else lo[l][DETAIL][j]
                    v = shrink(corrected(raw[f, j, rows, cols], (row, states)), LOW**l * HIGH, limit)
                    buf[f, k, rows, cols] = v
                    found.add((f, l), v)
            for (i, j), v in add_parts(lo, hi, upper_side, states, n4, n5, n6, f, rows, cols).items():
                if i == 0:
                    v = shrink(v, LOW**3 * HIGH, limit)
                    found.add((f, 3), v)
                (b4, m5, m6)[i][f, j, rows, cols] = v

        over_tiles(tile)
        for (f, l), part in found.parts.items():
            sums[f, l] = part

    @pl.when(upper)
    def _():
        outer_side(True)

    @pl.when(jnp.logical_not(upper))
    def _():
        outer_side(False)


def fifth(limits, outer5, inner, relayed, m5, m6, ends, sums_a, sums_b, b5, b6, total):
    upper, lowest, highest = where_am_i()
    lo, hi = response("lo")[4], response("hi")[4]
    found = Sums()

    def tile(f, rows, cols):
        limit = limits[f]
        below, above = [], []
        for k in range(2):
            o = outer5[f, k, rows, cols]
            n = inner[f, FAR + k, rows, cols] + relayed[f, k, rows, cols]
            e = ends[f, k, rows, cols]
            below.append(jnp.where(lowest, e, jnp.where(upper, n, o)))
            above.append(jnp.where(highest, e, jnp.where(upper, o, n)))
        for j in range(2):
            d = corrected(m5[f, j, rows, cols], (lo[DETAIL][j][FAR:], below), (hi[DETAIL][1 - j][FAR:], above))
            d = shrink(d, LOW**4 * HIGH, limit)
            b5[f, j, rows, cols] = d
            s = corrected(m6[f, j, rows, cols], (lo[APPROX][j][FAR:], below), (hi[APPROX][1 - j][FAR:], above))
            s = shrink(s, LOW**5, limit)
            b6[f, j, rows, cols] = s
            found.add((f, 0), d)
            found.add((f, 1), s)

    over_tiles(tile)
    lane = lax.broadcasted_iota(jnp.int32, (1, 128), 1)
    row = jnp.zeros((1, 128), jnp.float32)
    for f in range(2):
        for b in range(6):
            if b < 3:
                part = sums_a[f, b] + sums_b[f, b]
            elif b < 4:
                part = sums_b[f, b]
            else:
                part = found.parts[f, b - 4]
            row = row + jnp.where(lane == 6 * f + b, jnp.sum(part), 0.0)
    total[...] = row


def finish(cells, parts, b1, b2, b3, b4, b5, b6, o1_in, o2_in, o3_in, o1, o2, o3, o4, o5, o6, energy, row_vmem, sem):
    upper, _, _ = where_am_i()
    copies = [pltpu.make_async_copy(a, b, sem.at[k]) for k, (a, b) in enumerate(((b4, o4), (b5, o5), (b6, o6)))]
    for copy in copies:
        copy.start()

    def outer_side(upper_side):
        for f in range(2):
            for l, (buf, out) in enumerate(((b1, o1), (b2, o2), (b3, o3))):
                start, size = side(upper_side, l)
                yield pltpu.make_async_copy(
                    buf.at[f, pl.ds(0, size)], out.at[f, pl.ds(start, size)], sem.at[4 + 3 * f + l]
                )

    @pl.when(upper)
    def _():
        for copy in outer_side(True):
            copy.start()

    @pl.when(jnp.logical_not(upper))
    def _():
        for copy in outer_side(False):
            copy.start()

    row = jnp.sum(parts[...], axis=0) * (1.0 / cells[...])
    row_vmem[0:1, :] = row[:, 0:6]
    row_vmem[1:2, :] = row[:, 6:12]
    copies.append(pltpu.make_async_copy(row_vmem, energy, sem.at[3]))
    copies[-1].start()
    for copy in copies:
        copy.wait()

    @pl.when(upper)
    def _():
        for copy in outer_side(True):
            copy.wait()

    @pl.when(jnp.logical_not(upper))
    def _():
        for copy in outer_side(False):
            copy.wait()


def local(fields, threshold):
    f32 = jnp.float32
    vmem, hbm, smem = (pl.BlockSpec(memory_space=m) for m in (pltpu.VMEM, pltpu.HBM, pltpu.SMEM))

    def arr(n):
        return jax.ShapeDtypeStruct((2, n, 32, 256), f32)

    def tiles(n):
        return jax.ShapeDtypeStruct((2, n, 8, 128), f32)

    def buf(n):
        return pltpu.VMEM((2, n, 32, 256), f32)

    def call(body, ins, outs, scratch, flops, mib, aliases=None):
        return pl.pallas_call(
            body,
            in_specs=ins,
            out_specs=[s for s, _ in outs],
            out_shape=[a for _, a in outs],
            scratch_shapes=scratch,
            input_output_aliases=aliases or {},
            compiler_params=pltpu.CompilerParams(vmem_limit_bytes=mib << 20),
            cost_estimate=pl.CostEstimate(flops=flops, bytes_accessed=1 << 20, transcendentals=0),
        )

    count = lax.axis_size("gz")
    across = [(i, (i + 1) % count if i % 2 else (i - 1) % count) for i in range(count)]
    within = [(i, i ^ 1) for i in range(count)]

    states = jax.ShapeDtypeStruct((FAR, 32, 256), f32)
    kept = [(vmem, arr(n)) for n in (2, 2, ALL, 32, 16, 8, 4, 2, 2)]
    outer_a, *half, x_next = call(
        first_half,
        [hbm],
        [(vmem, states), *kept, (vmem, jax.ShapeDtypeStruct((64, 32, 256), f32))],
        [pltpu.VMEM((64, 32, 256), f32), pltpu.SemaphoreType.DMA((5,))],
        20_000_000,
        TRANSFORM_MIB,
    )(fields)
    outer_a = lax.ppermute(outer_a, "gz", across)
    outer_b, own5, passed, inner, d1, d2, d3, d4, d5, s5 = call(
        second_half, [vmem] * 10, [(vmem, states), *kept], [], 20_000_000, 4, {1 + k: 1 + k for k in range(9)}
    )(x_next, *half)
    passed = lax.ppermute(passed, "gz", within)
    outer_b = lax.ppermute(outer_b, "gz", across)
    (own5,) = call(hand_on, [vmem] * 2, [(vmem, arr(2))], [], 5_000_000, 4)(own5, passed)
    outer5 = lax.ppermute(own5, "gz", across)
    inner = lax.ppermute(inner, "gz", within)
    c1, c2, c3, sums_c = call(
        interiors,
        [smem] + [vmem] * 3,
        [(vmem, arr(n)) for n in (32, 16, 8)] + [(vmem, tiles(3))],
        [],
        20_000_000,
        4,
    )(threshold, d1, d2, d3)
    o1, o2, o3, n4, n5, n6, ends, sums_a = call(
        near,
        [smem] + [vmem] * 12,
        [(hbm, arr(32)), (hbm, arr(16)), (hbm, arr(8))] + [(vmem, arr(n)) for n in (4, 2, 2, 2)] + [(vmem, tiles(3))],
        [buf(3), buf(3), buf(3), pltpu.SemaphoreType.DMA((12,))],
        2_000_000_000,
        8,
    )(threshold, d1, d2, d3, d4, d5, s5, inner, own5, c1, c2, c3, sums_c)
    (relayed,) = call(hand_in, [vmem] * 3, [(vmem, arr(2))], [], 5_000_000, 4)(outer_a, outer_b, sums_a)
    received = lax.ppermute(relayed, "gz", within)
    b1, b2, b3, b4, m5, m6, sums_b = call(
        edges,
        [smem] + [vmem] * 9,
        [(vmem, arr(n)) for n in (2, 3, 3, 4, 2, 2)] + [(vmem, tiles(4))],
        [],
        1_000_000_000,
        4,
    )(threshold, outer_a, outer_b, d1, d2, d3, n4, n5, n6, relayed)
    b5, b6, total = call(
        fifth,
        [smem] + [vmem] * 8,
        [(vmem, arr(2)), (vmem, arr(2)), (vmem, jax.ShapeDtypeStruct((1, 128), f32))],
        [],
        5_000_000,
        4,
    )(threshold, outer5, inner, received, m5, m6, ends, sums_a, sums_b)

    devices = count * lax.axis_size("xy")
    parts = lax.all_to_all(jnp.broadcast_to(total, (devices, 1, 128)), ("gz", "xy"), 0, 0, tiled=True)
    cells = np.zeros((1, 128), np.float32) + 1.0
    cells[0, :12] = [n * 32 * 256 * devices for n in (32, 16, 8, 4, 2, 2)] * 2
    o1, o2, o3, o4, o5, o6, energy = call(
        finish,
        [vmem] * 8 + [hbm] * 3,
        [(hbm, arr(n)) for n in (32, 16, 8, 4, 2, 2)] + [(hbm, jax.ShapeDtypeStruct((2, 6), f32))],
        [pltpu.VMEM((2, 6), f32), pltpu.SemaphoreType.DMA((10,))],
        5_000_000,
        4,
        {8: 0, 9: 1, 10: 2},
    )(cells, parts, b1, b2, b3, b4, b5, b6, o1, o2, o3)
    return o1, o2, o3, o4, o5, o6, energy


def solution(mesh):
    split = P(None, "gz", "xy", None)

    def step(fields, threshold):
        return local(fields, threshold)

    step = jax.shard_map(step, mesh=mesh, in_specs=(split, P()), out_specs=(split,) * 6 + (P(),), check_vma=False)
    return step
```

```python
import functools

import jax
import jax.numpy as jnp
import numpy as np
from jax import lax
from jax.experimental import pallas as pl
from jax.experimental.pallas import tpu as pltpu
from jax.sharding import PartitionSpec as P


ALPHA = -1.586134342059924
BETA = -0.052980118572961
GAMMA = 0.882911075530934
DELTA = 0.443506852043971
KAPPA = 1.230174104914001
SQRT_TWO = 1.4142135623730951
LOW = SQRT_TWO / KAPPA
HIGH = KAPPA / SQRT_TWO
LEVELS = 5
FAR = 8
ALL = 2 * LEVELS
EDGE_LO = (1, 2, 3)
EDGE_HI = (2, 3, 3)


class Level:
    def __init__(self, n, left, right, emit_d, emit_s):
        self.n, self.left, self.right, self.emit_d, self.emit_s = n, left, right, emit_d, emit_s
        self.s, self.d, self.d1, self.s2, self.d3 = [], [], [], [], []

    def push(self, x):
        if len(self.s) == len(self.d):
            self.s.append(x)
            i = len(self.s) - 2
            if i >= 0:
                self.add(self.d[i] + ALPHA * (self.s[i] + self.s[i + 1]))
        else:
            self.d.append(x)
            if len(self.d) == self.n:
                self.finish()

    def add(self, v):
        self.d1.append(v)
        i = len(self.d1) - 1
        if i == 0:
            self.p = ALPHA * self.s[0]
            self.c = self.s[0] + BETA * v
            return
        if i == 1:
            a, b = self.left(self)
            below = a + self.p
            self.s2.append(self.c + BETA * below)
            self.d3m = below + GAMMA * ((b + BETA * below) + self.s2[0])
        if i == self.n - 1:
            self.s2.append(self.b + BETA * v)
        else:
            self.s2.append(self.s[i] + BETA * (self.d1[i - 1] + v))
        self.third(i - 1, self.s2[i])

    def third(self, j, above):
        self.d3.append(self.d1[j] + GAMMA * (self.s2[j] + above))
        self.emit_d(j, self.d3[j])
        before = self.d3[j - 1] if j else self.d3m
        self.emit_s(j, self.s2[j] + DELTA * (before + self.d3[j]))

    def finish(self):
        n = self.n
        self.a = self.d[n - 1] + ALPHA * self.s[n - 1]
        self.b = self.s[n - 1] + BETA * self.d1[n - 2]
        p, c = self.right(self)
        v = self.a + p
        self.add(v)
        self.third(n - 1, c + BETA * v)


def low_end(level):
    return level.d[0] + ALPHA * level.s[1], level.s[1] + BETA * level.d1[1]


def high_end(level):
    return ALPHA * level.s[-1], level.b


@functools.cache
def response(side, length=1024):
    zero, unit = np.zeros(2 * LEVELS), np.eye(2 * LEVELS)
    found, u = [], [zero] * length
    for l in range(LEVELS):
        n = len(u) // 2
        state, none = (unit[2 * l], unit[2 * l + 1]), (zero, zero)
        d, s = [None] * n, [None] * n
        level = Level(
            n,
            lambda _: state if side == "lo" else none,
            lambda _: state if side == "hi" else none,
            d.__setitem__,
            s.__setitem__,
        )
        for x in u:
            level.push(x)
        u = s
        down, up = (level.p, level.c), (level.a, level.b)
        found.append((down, up, d, s) if side == "lo" else (up, down, d[::-1], s[::-1]))
    return found


TRANSFORM_MIB = 46
BACK, ON, DETAIL, APPROX = range(4)


def combine(row, states):
    total = None
    for k, x in zip(row, states):
        if k != 0.0:
            term = float(k) * x
            total = term if total is None else total + term
    return total


def where_am_i():
    z = lax.axis_index("gz")
    return lax.rem(z, 2) == 1, z == 0, z == lax.axis_size("gz") - 1


def over_tiles(body, fields=(0, 1)):
    for f in fields:
        for rows in range(0, 32, 8):
            for cols in range(0, 256, 128):
                body(f, pl.ds(rows, 8), pl.ds(cols, 128))


class Sums:
    def __init__(self):
        self.parts = {}

    def add(self, key, v):
        self.parts[key] = self.parts[key] + v * v if key in self.parts else v * v


def first_half(x_hbm, outer, own5, passed, inner, d1, d2, d3, d4, d5, s5, x_next, x_vmem, sem):
    copies = []
    for j in range(4):
        rows = pl.ds(8 * j, 8)
        copies.append(pltpu.make_async_copy(x_hbm.at[0, :, rows], x_vmem.at[:, rows], sem.at[j]))
    copies.append(pltpu.make_async_copy(x_hbm.at[1], x_next, sem.at[4]))
    for copy in copies:
        copy.start()

    def fetched(j):
        rows = pl.ds(pl.multiple_of(8 * j, 8), 8)
        pltpu.make_async_copy(x_hbm.at[0, :, rows], x_vmem.at[:, rows], sem.at[j]).wait()

    transform(x_vmem, outer, own5, passed, inner, (d1, d2, d3, d4, d5), s5, 0, fetched)
    copies[4].wait()


def second_half(*refs):
    outer, own5, passed, inner, d1, d2, d3, d4, d5, s5 = refs[-10:]
    transform(refs[0], outer, own5, passed, inner, (d1, d2, d3, d4, d5), s5, 1, None)


def transform(x, outer, outer5, passed, inner, bands, s5, f, fetched):
    upper, lowest, highest = where_am_i()
    from_above, from_below = response("hi"), response("lo")

    def tile(i, carry):
        if fetched is not None:

            @pl.when(lax.rem(i, 2) == 0)
            def _():
                fetched(i // 2)

        rows = pl.ds(pl.multiple_of((i // 2) * 8, 8), 8)
        cols = pl.ds(pl.multiple_of(lax.rem(i, 2) * 128, 128), 128)
        down, up, levels = [], [], []

        def left(l):
            def state(level):
                down.extend((level.p, level.c))
                end = low_end(level)
                if l == 0:
                    return tuple(jnp.where(lowest, e, 0.0) for e in end)
                return tuple(jnp.where(lowest, e, combine(r, down)) for e, r in zip(end, from_above[l][BACK]))

            return state

        def right(l):
            def state(level):
                up.extend((level.a, level.b))
                end = high_end(level)
                if l == 0:
                    return tuple(jnp.where(highest, e, 0.0) for e in end)
                return tuple(jnp.where(highest, e, combine(r, up)) for e, r in zip(end, from_below[l][BACK]))

            return state

        def keep(l):
            def store(j, v):
                bands[l][f, j, rows, cols] = v

            return store

        def pass_on(l):
            def store(j, v):
                if l == LEVELS - 1:
                    s5[f, j, rows, cols] = v
                else:
                    levels[l + 1].push(v)

            return store

        for l in range(LEVELS):
            levels.append(Level(32 >> l, left(l), right(l), keep(l), pass_on(l)))
        for z in range(64):
            levels[0].push(x[z, rows, cols])
        for k in range(ALL):
            out = jnp.where(upper, up[k], down[k])
            if k < FAR:
                outer[k, rows, cols] = out
            else:
                outer5[f, k - FAR, rows, cols] = out
        inwards = [jnp.where(upper, y, x) for x, y in zip(up, down)]
        for k in range(ALL):
            inner[f, k, rows, cols] = inwards[k]
        for k, v in enumerate(through(inwards[:FAR], jnp.logical_not(upper))):
            passed[f, k, rows, cols] = v
        return carry

    lax.fori_loop(0, 8, tile, 0)


def shrink(v, scale, limit):
    v = v * scale
    return v - jnp.clip(v, -limit, limit)


def corrected(v, *parts):
    for row, states in parts:
        term = combine(row, states)
        if term is not None:
            v = term if v is None else v + term
    return v


def through(states, upper):
    lo, hi = response("lo", 64)[4][ON], response("hi", 64)[4][ON]
    sums = []
    for k in range(2):
        row = [jnp.where(upper, float(x), float(y)) for x, y in zip(lo[k], hi[k])]
        total = row[0] * states[0]
        for x, state in list(zip(row, states))[1:]:
            total = total + x * state
        sums.append(total)
    return sums


def hand_on(own5, passed, out5):
    out5[...] = own5[...] + passed[...]


def hand_in(outer_a, outer_b, after, out5):
    upper, lowest, highest = where_am_i()
    end = jnp.logical_or(lowest, highest)

    def tile(f, rows, cols):
        extra = through([(outer_a, outer_b)[f][k, rows, cols] for k in range(FAR)], jnp.logical_not(upper))
        for k in range(2):
            out5[f, k, rows, cols] = jnp.where(end, 0.0, extra[k])

    over_tiles(tile)


def add_parts(lo, hi, upper_side, states, v4, v5, v6, f, rows, cols):
    rows_of, sums = (hi if upper_side else lo), {}
    for i, (src, l, kind, n) in enumerate(((v4, 3, DETAIL, 4), (v5, 4, DETAIL, 2), (v6, 4, APPROX, 2))):
        for j in range(n):
            row = rows_of[l][kind][n - 1 - j if upper_side else j][:FAR]
            sums[i, j] = corrected(src[f, j, rows, cols], (row, states))
    return sums


def side(upper_side, l):
    return ((32 >> l) - EDGE_HI[l], EDGE_HI[l]) if upper_side else (0, EDGE_LO[l])


def interiors(limits, d1, d2, d3, o1, o2, o3, sums, limit_tiles, b1, b2, b3, sem):
    copies = []
    for f in range(2):
        limit_tiles[f] = jnp.full((8, 128), limits[f], jnp.float32)
    for l, (raw, buf, out) in enumerate(((d1, b1, o1), (d2, b2, o2), (d3, b3, o3))):
        first, last = EDGE_LO[l], (32 >> l) - EDGE_HI[l]
        for f in range(2):
            limit = limits[f]

            def layer(z, total, raw=raw, buf=buf, l=l, f=f, limit=limit):
                v = shrink(raw[f, z], LOW**l * HIGH, limit)
                buf[f, z] = v
                return total + v * v

            total = lax.fori_loop(first, last, layer, jnp.zeros((32, 256), jnp.float32), unroll=True)
            at = (f, pl.ds(first, last - first))
            copy = pltpu.make_async_copy(buf.at[at], out.at[at], sem.at[3 * f + l])
            copy.start()
            copies.append(copy)
            total = total.reshape(4, 8, 256).sum(axis=0)
            sums[f, l] = total[:, :128] + total[:, 128:]
    for copy in copies:
        copy.wait()


def pieces(pairs, upper_side, sem, base):
    for f in range(2):
        for l, (buf, out) in enumerate(pairs):
            start, size = side(upper_side, l)
            yield pltpu.make_async_copy(
                buf.at[f, pl.ds(0, size)], out.at[f, pl.ds(start, size)], sem.at[base + 3 * f + l]
            )


def near(limits, d1, d2, d3, d4, d5, s5, inner, after, acc, e1, e2, e3, n4, n5, n6, ends, sums):
    upper, lowest, highest = where_am_i()
    lo, hi = response("lo"), response("hi")
    pass_up = response("lo", 64)[4][ON]
    triples = ((d1, e1), (d2, e2), (d3, e3))

    def inner_side(upper_side):
        found = Sums()

        def tile(f, rows, cols):
            limit = limits[f]
            states = [inner[f, k, rows, cols] for k in range(FAR)]
            for l, (raw, buf) in enumerate(triples):
                start, size = side(upper_side, l)
                for k in range(size):
                    j = start + k
                    row = hi[l][DETAIL][(32 >> l) - 1 - j] if upper_side else lo[l][DETAIL][j]
                    v = shrink(corrected(raw[f, j, rows, cols], (row, states)), LOW**l * HIGH, limit)
                    buf[f, k, rows, cols] = v
                    found.add((f, l), v)
            for (l, j), v in add_parts(lo, hi, upper_side, states, d4, d5, s5, f, rows, cols).items():
                (n4, n5, n6)[l][f, j, rows, cols] = v

        over_tiles(tile)
        for (f, l), part in found.parts.items():
            sums[f, l] = acc[f, l] + part

    @pl.when(jnp.logical_not(jnp.logical_or(lowest, highest)))
    def _():
        ends[...] = jnp.zeros(ends.shape, jnp.float32)

    @pl.when(lowest)
    def _():
        def tile(f, rows, cols):
            above = [inner[f, k, rows, cols] for k in range(FAR)]
            u = [combine(hi[3][APPROX][3 - j], above) for j in range(4)]
            ends[f, 0, rows, cols] = u[1] + ALPHA * u[2]
            ends[f, 1, rows, cols] = u[2] + BETA * ((u[3] + ALPHA * u[2]) + inner[f, FAR, rows, cols])

        over_tiles(tile)

    @pl.when(highest)
    def _():
        def tile(f, rows, cols):
            below = [inner[f, k, rows, cols] for k in range(FAR)]
            ends[f, 0, rows, cols] = ALPHA * combine(lo[3][APPROX][2], below)
            ends[f, 1, rows, cols] = combine(pass_up[1], below)

        over_tiles(tile)

    @pl.when(upper)
    def _():
        inner_side(False)

    @pl.when(jnp.logical_not(upper))
    def _():
        inner_side(True)


def edges(
    limits, outer_a, outer_b, d1, d2, d3, n4, n5, n6, after, e1, e2, e3, o1_in, o2_in, o3_in,
    b1, b2, b3, b4, m5, m6, sums, o1, o2, o3, sem,
):
    upper, lowest, highest = where_am_i()
    end = jnp.logical_or(lowest, highest)
    lo, hi = response("lo"), response("hi")

    def outer_side(upper_side):
        found = Sums()
        copies = [*pieces(((e1, o1), (e2, o2), (e3, o3)), not upper_side, sem, 0)]
        for copy in copies:
            copy.start()

        def tile(f, rows, cols):
            limit = limits[f]
            states = [jnp.where(end, 0.0, (outer_a, outer_b)[f][k, rows, cols]) for k in range(FAR)]
            for l, (raw, buf) in enumerate(((d1, b1), (d2, b2), (d3, b3))):
                start, size = side(upper_side, l)
                for k in range(size):
                    j = start + k
                    row = hi[l][DETAIL][(32 >> l) - 1 - j] if upper_side else lo[l][DETAIL][j]
                    v = shrink(corrected(raw[f, j, rows, cols], (row, states)), LOW**l * HIGH, limit)
                    buf[f, k, rows, cols] = v
                    found.add((f, l), v)
            for (i, j), v in add_parts(lo, hi, upper_side, states, n4, n5, n6, f, rows, cols).items():
                if i == 0:
                    v = shrink(v, LOW**3 * HIGH, limit)
                    found.add((f, 3), v)
                (b4, m5, m6)[i][f, j, rows, cols] = v

        over_tiles(tile)
        for (f, l), part in found.parts.items():
            sums[f, l] = part
        for copy in copies:
            copy.wait()

    @pl.when(upper)
    def _():
        outer_side(True)

    @pl.when(jnp.logical_not(upper))
    def _():
        outer_side(False)


def total_of(part):
    return jnp.sum(jnp.sum(part, axis=0, keepdims=True), axis=1, keepdims=True)


def fifth(limits, outer5, inner, relayed, m5, m6, ends, sums_a, sums_b, b5, b6, total):
    upper, lowest, highest = where_am_i()
    lo, hi = response("lo")[4], response("hi")[4]
    found = Sums()

    def tile(f, rows, cols):
        limit = limits[f]
        below, above = [], []
        for k in range(2):
            o = outer5[f, k, rows, cols]
            n = inner[f, FAR + k, rows, cols] + relayed[f, k, rows, cols]
            e = ends[f, k, rows, cols]
            below.append(jnp.where(lowest, e, jnp.where(upper, n, o)))
            above.append(jnp.where(highest, e, jnp.where(upper, o, n)))
        for j in range(2):
            d = corrected(m5[f, j, rows, cols], (lo[DETAIL][j][FAR:], below), (hi[DETAIL][1 - j][FAR:], above))
            d = shrink(d, LOW**4 * HIGH, limit)
            b5[f, j, rows, cols] = d
            s = corrected(m6[f, j, rows, cols], (lo[APPROX][j][FAR:], below), (hi[APPROX][1 - j][FAR:], above))
            s = shrink(s, LOW**5, limit)
            b6[f, j, rows, cols] = s
            found.add((f, 0), d)
            found.add((f, 1), s)

    over_tiles(tile)
    lane = lax.broadcasted_iota(jnp.int32, (1, 128), 1)
    row = jnp.zeros((1, 128), jnp.float32)
    for f in range(2):
        for b in range(6):
            if b < 3:
                part = sums_a[f, b] + sums_b[f, b]
            elif b < 4:
                part = sums_b[f, b]
            else:
                part = found.parts[f, b - 4]
            row = row + jnp.where(lane == 6 * f + b, total_of(part), 0.0)
    total[...] = row


def finish(cells, parts, b1, b2, b3, b4, b5, b6, o1_in, o2_in, o3_in, o1, o2, o3, o4, o5, o6, energy, row_vmem, sem):
    upper, _, _ = where_am_i()
    copies = [pltpu.make_async_copy(a, b, sem.at[k]) for k, (a, b) in enumerate(((b4, o4), (b5, o5), (b6, o6)))]
    for copy in copies:
        copy.start()

    def outer_side(upper_side):
        return pieces(((b1, o1), (b2, o2), (b3, o3)), upper_side, sem, 4)

    @pl.when(upper)
    def _():
        for copy in outer_side(True):
            copy.start()

    @pl.when(jnp.logical_not(upper))
    def _():
        for copy in outer_side(False):
            copy.start()

    row = jnp.sum(parts[...], axis=0) * (1.0 / cells[...])
    row_vmem[0:1, :] = row[:, 0:6]
    row_vmem[1:2, :] = row[:, 6:12]
    copies.append(pltpu.make_async_copy(row_vmem, energy, sem.at[3]))
    copies[-1].start()
    for copy in copies:
        copy.wait()

    @pl.when(upper)
    def _():
        for copy in outer_side(True):
            copy.wait()

    @pl.when(jnp.logical_not(upper))
    def _():
        for copy in outer_side(False):
            copy.wait()


def local(fields, threshold):
    f32 = jnp.float32
    vmem, hbm, smem = (pl.BlockSpec(memory_space=m) for m in (pltpu.VMEM, pltpu.HBM, pltpu.SMEM))

    def arr(n):
        return jax.ShapeDtypeStruct((2, n, 32, 256), f32)

    def tiles(n):
        return jax.ShapeDtypeStruct((2, n, 8, 128), f32)

    def buf(n):
        return pltpu.VMEM((2, n, 32, 256), f32)

    def call(body, ins, outs, scratch, flops, mib, aliases=None):
        return pl.pallas_call(
            body,
            in_specs=ins,
            out_specs=[s for s, _ in outs],
            out_shape=[a for _, a in outs],
            scratch_shapes=scratch,
            input_output_aliases=aliases or {},
            compiler_params=pltpu.CompilerParams(vmem_limit_bytes=mib << 20),
            cost_estimate=pl.CostEstimate(flops=flops, bytes_accessed=1 << 20, transcendentals=0),
        )

    count = lax.axis_size("gz")
    across = [(i, (i + 1) % count if i % 2 else (i - 1) % count) for i in range(count)]
    within = [(i, i ^ 1) for i in range(count)]

    states = jax.ShapeDtypeStruct((FAR, 32, 256), f32)
    kept = [(vmem, arr(n)) for n in (2, 2, ALL, 32, 16, 8, 4, 2, 2)]
    outer_a, *half, x_next = call(
        first_half,
        [hbm],
        [(vmem, states), *kept, (vmem, jax.ShapeDtypeStruct((64, 32, 256), f32))],
        [pltpu.VMEM((64, 32, 256), f32), pltpu.SemaphoreType.DMA((5,))],
        20_000_000,
        TRANSFORM_MIB,
    )(fields)
    outer_a = lax.ppermute(outer_a, "gz", across)
    outer_b, own5, passed, inner, d1, d2, d3, d4, d5, s5 = call(
        second_half, [vmem] * 10, [(vmem, states), *kept], [], 20_000_000, 4, {1 + k: 1 + k for k in range(9)}
    )(x_next, *half)
    passed = lax.ppermute(passed, "gz", within)
    outer_b = lax.ppermute(outer_b, "gz", across)
    (own5,) = call(hand_on, [vmem] * 2, [(vmem, arr(2))], [], 5_000_000, 4)(own5, passed)
    outer5 = lax.ppermute(own5, "gz", across)
    inner = lax.ppermute(inner, "gz", within)
    o1, o2, o3, sums_c, limits = call(
        interiors,
        [smem] + [vmem] * 3,
        [(hbm, arr(n)) for n in (32, 16, 8)] + [(vmem, tiles(3)), (vmem, jax.ShapeDtypeStruct((2, 8, 128), f32))],
        [buf(32), buf(16), buf(8), pltpu.SemaphoreType.DMA((6,))],
        20_000_000,
        8,
    )(threshold, d1, d2, d3)
    e1, e2, e3, n4, n5, n6, ends, sums_a = call(
        near,
        [vmem] * 10,
        [(vmem, arr(n)) for n in (3, 3, 3, 4, 2, 2, 2)] + [(vmem, tiles(3))],
        [],
        2_000_000_000,
        4,
    )(limits, d1, d2, d3, d4, d5, s5, inner, own5, sums_c)
    (relayed,) = call(hand_in, [vmem] * 3, [(vmem, arr(2))], [], 5_000_000, 4)(outer_a, outer_b, sums_a)
    received = lax.ppermute(relayed, "gz", within)
    b1, b2, b3, b4, m5, m6, sums_b, o1, o2, o3 = call(
        edges,
        [vmem] * 13 + [hbm] * 3,
        [(vmem, arr(n)) for n in (2, 3, 3, 4, 2, 2)] + [(vmem, tiles(4))] + [(hbm, arr(n)) for n in (32, 16, 8)],
        [pltpu.SemaphoreType.DMA((6,))],
        1_000_000_000,
        4,
        {13: 7, 14: 8, 15: 9},
    )(limits, outer_a, outer_b, d1, d2, d3, n4, n5, n6, relayed, e1, e2, e3, o1, o2, o3)
    b5, b6, total = call(
        fifth,
        [vmem] * 9,
        [(vmem, arr(2)), (vmem, arr(2)), (vmem, jax.ShapeDtypeStruct((1, 128), f32))],
        [],
        5_000_000,
        4,
    )(limits, outer5, inner, received, m5, m6, ends, sums_a, sums_b)

    devices = count * lax.axis_size("xy")
    parts = lax.all_to_all(jnp.broadcast_to(total, (devices, 1, 128)), ("gz", "xy"), 0, 0, tiled=True)
    cells = np.zeros((1, 128), np.float32) + 1.0
    cells[0, :12] = [n * 32 * 256 * devices for n in (32, 16, 8, 4, 2, 2)] * 2
    o1, o2, o3, o4, o5, o6, energy = call(
        finish,
        [vmem] * 8 + [hbm] * 3,
        [(hbm, arr(n)) for n in (32, 16, 8, 4, 2, 2)] + [(hbm, jax.ShapeDtypeStruct((2, 6), f32))],
        [pltpu.VMEM((2, 6), f32), pltpu.SemaphoreType.DMA((10,))],
        5_000_000,
        4,
        {8: 0, 9: 1, 10: 2},
    )(cells, parts, b1, b2, b3, b4, b5, b6, o1, o2, o3)
    return o1, o2, o3, o4, o5, o6, energy


def solution(mesh):
    split = P(None, "gz", "xy", None)

    def step(fields, threshold):
        return local(fields, threshold)

    step = jax.shard_map(step, mesh=mesh, in_specs=(split, P()), out_specs=(split,) * 6 + (P(),), check_vma=False)
    return step
```

```python
import functools

import jax
import jax.numpy as jnp
import numpy as np
from jax import lax
from jax.experimental import pallas as pl
from jax.experimental.pallas import tpu as pltpu
from jax.sharding import PartitionSpec as P


ALPHA = -1.586134342059924
BETA = -0.052980118572961
GAMMA = 0.882911075530934
DELTA = 0.443506852043971
KAPPA = 1.230174104914001
SQRT_TWO = 1.4142135623730951
LOW = SQRT_TWO / KAPPA
HIGH = KAPPA / SQRT_TWO
LEVELS = 5
FAR = 8
ALL = 2 * LEVELS
EDGE_LO = (1, 2, 3)
EDGE_HI = (2, 3, 3)


class Level:
    def __init__(self, n, left, right, emit_d, emit_s):
        self.n, self.left, self.right, self.emit_d, self.emit_s = n, left, right, emit_d, emit_s
        self.s, self.d, self.d1, self.s2, self.d3 = [], [], [], [], []

    def push(self, x):
        if len(self.s) == len(self.d):
            self.s.append(x)
            i = len(self.s) - 2
            if i >= 0:
                self.add(self.d[i] + ALPHA * (self.s[i] + self.s[i + 1]))
        else:
            self.d.append(x)
            if len(self.d) == self.n:
                self.finish()

    def add(self, v):
        self.d1.append(v)
        i = len(self.d1) - 1
        if i == 0:
            self.p = ALPHA * self.s[0]
            self.c = self.s[0] + BETA * v
            return
        if i == 1:
            a, b = self.left(self)
            below = a + self.p
            self.s2.append(self.c + BETA * below)
            self.d3m = below + GAMMA * ((b + BETA * below) + self.s2[0])
        if i == self.n - 1:
            self.s2.append(self.b + BETA * v)
        else:
            self.s2.append(self.s[i] + BETA * (self.d1[i - 1] + v))
        self.third(i - 1, self.s2[i])

    def third(self, j, above):
        self.d3.append(self.d1[j] + GAMMA * (self.s2[j] + above))
        self.emit_d(j, self.d3[j])
        before = self.d3[j - 1] if j else self.d3m
        self.emit_s(j, self.s2[j] + DELTA * (before + self.d3[j]))

    def finish(self):
        n = self.n
        self.a = self.d[n - 1] + ALPHA * self.s[n - 1]
        self.b = self.s[n - 1] + BETA * self.d1[n - 2]
        p, c = self.right(self)
        v = self.a + p
        self.add(v)
        self.third(n - 1, c + BETA * v)


def low_end(level):
    return level.d[0] + ALPHA * level.s[1], level.s[1] + BETA * level.d1[1]


def high_end(level):
    return ALPHA * level.s[-1], level.b


@functools.cache
def response(side, length=1024):
    zero, unit = np.zeros(2 * LEVELS), np.eye(2 * LEVELS)
    found, u = [], [zero] * length
    for l in range(LEVELS):
        n = len(u) // 2
        state, none = (unit[2 * l], unit[2 * l + 1]), (zero, zero)
        d, s = [None] * n, [None] * n
        level = Level(
            n,
            lambda _: state if side == "lo" else none,
            lambda _: state if side == "hi" else none,
            d.__setitem__,
            s.__setitem__,
        )
        for x in u:
            level.push(x)
        u = s
        down, up = (level.p, level.c), (level.a, level.b)
        found.append((down, up, d, s) if side == "lo" else (up, down, d[::-1], s[::-1]))
    return found


TRANSFORM_MIB = 46
BACK, ON, DETAIL, APPROX = range(4)


def combine(row, states):
    total = None
    for k, x in zip(row, states):
        if k != 0.0:
            term = float(k) * x
            total = term if total is None else total + term
    return total


def where_am_i():
    z = lax.axis_index("gz")
    return lax.rem(z, 2) == 1, z == 0, z == lax.axis_size("gz") - 1


def over_tiles(body, fields=(0, 1)):
    for f in fields:
        for rows in range(0, 32, 8):
            for cols in range(0, 256, 128):
                body(f, pl.ds(rows, 8), pl.ds(cols, 128))


class Sums:
    def __init__(self):
        self.parts = {}

    def add(self, key, v):
        self.parts[key] = self.parts[key] + v * v if key in self.parts else v * v


def first_half(x_hbm, outer, own5, passed, inner, d1, d2, d3, d4, d5, s5, x_next, x_vmem, sem):
    copies = []
    for j in range(4):
        rows = pl.ds(8 * j, 8)
        copies.append(pltpu.make_async_copy(x_hbm.at[0, :, rows], x_vmem.at[:, rows], sem.at[j]))
    copies.append(pltpu.make_async_copy(x_hbm.at[1], x_next, sem.at[4]))
    for copy in copies:
        copy.start()

    def fetched(j):
        rows = pl.ds(pl.multiple_of(8 * j, 8), 8)
        pltpu.make_async_copy(x_hbm.at[0, :, rows], x_vmem.at[:, rows], sem.at[j]).wait()

    transform(x_vmem, outer, own5, passed, inner, (d1, d2, d3, d4, d5), s5, 0, fetched)
    copies[4].wait()


def second_half(*refs):
    outer, own5, passed, inner, d1, d2, d3, d4, d5, s5 = refs[-10:]
    transform(refs[0], outer, own5, passed, inner, (d1, d2, d3, d4, d5), s5, 1, None)


def transform(x, outer, outer5, passed, inner, bands, s5, f, fetched):
    upper, lowest, highest = where_am_i()
    from_above, from_below = response("hi"), response("lo")

    def tile(i, carry):
        if fetched is not None:

            @pl.when(lax.rem(i, 2) == 0)
            def _():
                fetched(i // 2)

        rows = pl.ds(pl.multiple_of((i // 2) * 8, 8), 8)
        cols = pl.ds(pl.multiple_of(lax.rem(i, 2) * 128, 128), 128)
        down, up, levels = [], [], []

        def left(l):
            def state(level):
                down.extend((level.p, level.c))
                end = low_end(level)
                if l == 0:
                    return tuple(jnp.where(lowest, e, 0.0) for e in end)
                return tuple(jnp.where(lowest, e, combine(r, down)) for e, r in zip(end, from_above[l][BACK]))

            return state

        def right(l):
            def state(level):
                up.extend((level.a, level.b))
                end = high_end(level)
                if l == 0:
                    return tuple(jnp.where(highest, e, 0.0) for e in end)
                return tuple(jnp.where(highest, e, combine(r, up)) for e, r in zip(end, from_below[l][BACK]))

            return state

        def keep(l):
            def store(j, v):
                bands[l][f, j, rows, cols] = v

            return store

        def pass_on(l):
            def store(j, v):
                if l == LEVELS - 1:
                    s5[f, j, rows, cols] = v
                else:
                    levels[l + 1].push(v)

            return store

        for l in range(LEVELS):
            levels.append(Level(32 >> l, left(l), right(l), keep(l), pass_on(l)))
        for z in range(64):
            levels[0].push(x[z, rows, cols])
        for k in range(ALL):
            out = jnp.where(upper, up[k], down[k])
            if k < FAR:
                outer[k, rows, cols] = out
            else:
                outer5[f, k - FAR, rows, cols] = out
        inwards = [jnp.where(upper, y, x) for x, y in zip(up, down)]
        for k in range(ALL):
            inner[f, k, rows, cols] = inwards[k]
        for k, v in enumerate(through(inwards[:FAR], jnp.logical_not(upper))):
            passed[f, k, rows, cols] = v
        return carry

    lax.fori_loop(0, 8, tile, 0)


def shrink(v, scale, limit):
    v = v * scale
    return v - jnp.clip(v, -limit, limit)


def corrected(v, *parts):
    for row, states in parts:
        term = combine(row, states)
        if term is not None:
            v = term if v is None else v + term
    return v


def through(states, upper):
    lo, hi = response("lo", 64)[4][ON], response("hi", 64)[4][ON]
    sums = []
    for k in range(2):
        row = [jnp.where(upper, float(x), float(y)) for x, y in zip(lo[k], hi[k])]
        total = row[0] * states[0]
        for x, state in list(zip(row, states))[1:]:
            total = total + x * state
        sums.append(total)
    return sums


def hand_on(own5, passed, out5):
    out5[...] = own5[...] + passed[...]


def hand_in(outer_a, outer_b, after, out5):
    upper, lowest, highest = where_am_i()
    end = jnp.logical_or(lowest, highest)

    def tile(f, rows, cols):
        extra = through([(outer_a, outer_b)[f][k, rows, cols] for k in range(FAR)], jnp.logical_not(upper))
        for k in range(2):
            out5[f, k, rows, cols] = jnp.where(end, 0.0, extra[k])

    over_tiles(tile)


def add_parts(lo, hi, upper_side, states, v4, v5, v6, f, rows, cols):
    rows_of, sums = (hi if upper_side else lo), {}
    for i, (src, l, kind, n) in enumerate(((v4, 3, DETAIL, 4), (v5, 4, DETAIL, 2), (v6, 4, APPROX, 2))):
        for j in range(n):
            row = rows_of[l][kind][n - 1 - j if upper_side else j][:FAR]
            sums[i, j] = corrected(src[f, j, rows, cols], (row, states))
    return sums


def side(upper_side, l):
    return ((32 >> l) - EDGE_HI[l], EDGE_HI[l]) if upper_side else (0, EDGE_LO[l])


def interiors(limits, d1, d2, d3, o1, o2, o3, sums, limit_tiles, b1, b2, b3, sem):
    copies = []
    for f in range(2):
        limit_tiles[f] = jnp.full((8, 128), limits[f], jnp.float32)
    for l, (raw, buf, out) in enumerate(((d1, b1, o1), (d2, b2, o2), (d3, b3, o3))):
        first, last = EDGE_LO[l], (32 >> l) - EDGE_HI[l]
        for f in range(2):
            limit = limits[f]

            def layer(z, total, raw=raw, buf=buf, l=l, f=f, limit=limit):
                v = shrink(raw[f, z], LOW**l * HIGH, limit)
                buf[f, z] = v
                return total + v * v

            total = lax.fori_loop(first, last, layer, jnp.zeros((32, 256), jnp.float32), unroll=True)
            at = (f, pl.ds(first, last - first))
            copy = pltpu.make_async_copy(buf.at[at], out.at[at], sem.at[3 * f + l])
            copy.start()
            copies.append(copy)
            total = total.reshape(4, 8, 256).sum(axis=0)
            sums[f, l] = total[:, :128] + total[:, 128:]
    for copy in copies:
        copy.wait()


def pieces(pairs, upper_side, sem, base):
    for f in range(2):
        for l, (buf, out) in enumerate(pairs):
            start, size = side(upper_side, l)
            yield pltpu.make_async_copy(
                buf.at[f, pl.ds(0, size)], out.at[f, pl.ds(start, size)], sem.at[base + 3 * f + l]
            )


def near(limits, d1, d2, d3, d4, d5, s5, inner, after, acc, e1, e2, e3, n4, n5, n6, ends, sums):
    upper, lowest, highest = where_am_i()
    lo, hi = response("lo"), response("hi")
    pass_up = response("lo", 64)[4][ON]
    triples = ((d1, e1), (d2, e2), (d3, e3))

    def inner_side(upper_side):
        found = Sums()

        def tile(f, rows, cols):
            limit = limits[f]
            states = [inner[f, k, rows, cols] for k in range(FAR)]
            for l, (raw, buf) in enumerate(triples):
                start, size = side(upper_side, l)
                for k in range(size):
                    j = start + k
                    row = hi[l][DETAIL][(32 >> l) - 1 - j] if upper_side else lo[l][DETAIL][j]
                    v = shrink(corrected(raw[f, j, rows, cols], (row, states)), LOW**l * HIGH, limit)
                    buf[f, k, rows, cols] = v
                    found.add((f, l), v)
            for (l, j), v in add_parts(lo, hi, upper_side, states, d4, d5, s5, f, rows, cols).items():
                (n4, n5, n6)[l][f, j, rows, cols] = v

        over_tiles(tile)
        for (f, l), part in found.parts.items():
            sums[f, l] = acc[f, l] + part

    @pl.when(jnp.logical_not(jnp.logical_or(lowest, highest)))
    def _():
        ends[...] = jnp.zeros(ends.shape, jnp.float32)

    @pl.when(lowest)
    def _():
        def tile(f, rows, cols):
            above = [inner[f, k, rows, cols] for k in range(FAR)]
            u = [combine(hi[3][APPROX][3 - j], above) for j in range(4)]
            ends[f, 0, rows, cols] = u[1] + ALPHA * u[2]
            ends[f, 1, rows, cols] = u[2] + BETA * ((u[3] + ALPHA * u[2]) + inner[f, FAR, rows, cols])

        over_tiles(tile)

    @pl.when(highest)
    def _():
        def tile(f, rows, cols):
            below = [inner[f, k, rows, cols] for k in range(FAR)]
            ends[f, 0, rows, cols] = ALPHA * combine(lo[3][APPROX][2], below)
            ends[f, 1, rows, cols] = combine(pass_up[1], below)

        over_tiles(tile)

    @pl.when(upper)
    def _():
        inner_side(False)

    @pl.when(jnp.logical_not(upper))
    def _():
        inner_side(True)


def edges(
    limits, outer_a, outer_b, d1, d2, d3, n4, n5, n6, after, e1, e2, e3, o1_in, o2_in, o3_in,
    m5, m6, sums, o1, o2, o3, o4, b1, b2, b3, b4, sem,
):
    upper, lowest, highest = where_am_i()
    end = jnp.logical_or(lowest, highest)
    lo, hi = response("lo"), response("hi")

    def outer_side(upper_side):
        found = Sums()
        copies = [*pieces(((e1, o1), (e2, o2), (e3, o3)), not upper_side, sem, 0)]
        for copy in copies:
            copy.start()

        def tile(f, rows, cols):
            limit = limits[f]
            states = [jnp.where(end, 0.0, (outer_a, outer_b)[f][k, rows, cols]) for k in range(FAR)]
            for l, (raw, buf) in enumerate(((d1, b1), (d2, b2), (d3, b3))):
                start, size = side(upper_side, l)
                for k in range(size):
                    j = start + k
                    row = hi[l][DETAIL][(32 >> l) - 1 - j] if upper_side else lo[l][DETAIL][j]
                    v = shrink(corrected(raw[f, j, rows, cols], (row, states)), LOW**l * HIGH, limit)
                    buf[f, k, rows, cols] = v
                    found.add((f, l), v)
            for (i, j), v in add_parts(lo, hi, upper_side, states, n4, n5, n6, f, rows, cols).items():
                if i == 0:
                    v = shrink(v, LOW**3 * HIGH, limit)
                    found.add((f, 3), v)
                (b4, m5, m6)[i][f, j, rows, cols] = v

        own = [*pieces(((b1, o1), (b2, o2), (b3, o3)), upper_side, sem, 6)]
        for f in range(2):
            over_tiles(tile, (f,))
            done = own[3 * f : 3 * f + 3] + [pltpu.make_async_copy(b4.at[f], o4.at[f], sem.at[12 + f])]
            for copy in done:
                copy.start()
            copies += done
        for (f, l), part in found.parts.items():
            sums[f, l] = part
        for copy in copies:
            copy.wait()

    @pl.when(upper)
    def _():
        outer_side(True)

    @pl.when(jnp.logical_not(upper))
    def _():
        outer_side(False)


def total_of(part):
    return jnp.sum(jnp.sum(part, axis=0, keepdims=True), axis=1, keepdims=True)


def fifth(limits, outer5, inner, relayed, m5, m6, ends, sums_a, sums_b, b5, b6, total):
    upper, lowest, highest = where_am_i()
    lo, hi = response("lo")[4], response("hi")[4]
    found = Sums()

    def tile(f, rows, cols):
        limit = limits[f]
        below, above = [], []
        for k in range(2):
            o = outer5[f, k, rows, cols]
            n = inner[f, FAR + k, rows, cols] + relayed[f, k, rows, cols]
            e = ends[f, k, rows, cols]
            below.append(jnp.where(lowest, e, jnp.where(upper, n, o)))
            above.append(jnp.where(highest, e, jnp.where(upper, o, n)))
        for j in range(2):
            d = corrected(m5[f, j, rows, cols], (lo[DETAIL][j][FAR:], below), (hi[DETAIL][1 - j][FAR:], above))
            d = shrink(d, LOW**4 * HIGH, limit)
            b5[f, j, rows, cols] = d
            s = corrected(m6[f, j, rows, cols], (lo[APPROX][j][FAR:], below), (hi[APPROX][1 - j][FAR:], above))
            s = shrink(s, LOW**5, limit)
            b6[f, j, rows, cols] = s
            found.add((f, 0), d)
            found.add((f, 1), s)

    over_tiles(tile)
    lane = lax.broadcasted_iota(jnp.int32, (1, 128), 1)
    row = jnp.zeros((1, 128), jnp.float32)
    for f in range(2):
        for b in range(6):
            if b < 3:
                part = sums_a[f, b] + sums_b[f, b]
            elif b < 4:
                part = sums_b[f, b]
            else:
                part = found.parts[f, b - 4]
            row = row + jnp.where(lane == 6 * f + b, total_of(part), 0.0)
    total[...] = row


def finish(cells, parts, b5, b6, o5, o6, energy, row_vmem, sem):
    copies = [pltpu.make_async_copy(a, b, sem.at[k]) for k, (a, b) in enumerate(((b5, o5), (b6, o6)))]
    for copy in copies:
        copy.start()
    some = [jnp.sum(parts[k : k + 32], axis=0) for k in range(0, parts.shape[0], 32)]
    while len(some) > 1:
        some = [a + b for a, b in zip(some[::2], some[1::2])]
    row = some[0] * (1.0 / cells[...])
    row_vmem[0:1, :] = row[:, 0:6]
    row_vmem[1:2, :] = row[:, 6:12]
    copies.append(pltpu.make_async_copy(row_vmem, energy, sem.at[2]))
    copies[-1].start()
    for copy in copies:
        copy.wait()


def local(fields, threshold):
    f32 = jnp.float32
    vmem, hbm, smem = (pl.BlockSpec(memory_space=m) for m in (pltpu.VMEM, pltpu.HBM, pltpu.SMEM))

    def arr(n):
        return jax.ShapeDtypeStruct((2, n, 32, 256), f32)

    def tiles(n):
        return jax.ShapeDtypeStruct((2, n, 8, 128), f32)

    def buf(n):
        return pltpu.VMEM((2, n, 32, 256), f32)

    def call(body, ins, outs, scratch, flops, mib, aliases=None):
        return pl.pallas_call(
            body,
            in_specs=ins,
            out_specs=[s for s, _ in outs],
            out_shape=[a for _, a in outs],
            scratch_shapes=scratch,
            input_output_aliases=aliases or {},
            compiler_params=pltpu.CompilerParams(vmem_limit_bytes=mib << 20),
            cost_estimate=pl.CostEstimate(flops=flops, bytes_accessed=1 << 20, transcendentals=0),
        )

    count = lax.axis_size("gz")
    across = [(i, (i + 1) % count if i % 2 else (i - 1) % count) for i in range(count)]
    within = [(i, i ^ 1) for i in range(count)]

    states = jax.ShapeDtypeStruct((FAR, 32, 256), f32)
    kept = [(vmem, arr(n)) for n in (2, 2, ALL, 32, 16, 8, 4, 2, 2)]
    outer_a, *half, x_next = call(
        first_half,
        [hbm],
        [(vmem, states), *kept, (vmem, jax.ShapeDtypeStruct((64, 32, 256), f32))],
        [pltpu.VMEM((64, 32, 256), f32), pltpu.SemaphoreType.DMA((5,))],
        20_000_000,
        TRANSFORM_MIB,
    )(fields)
    outer_a = lax.ppermute(outer_a, "gz", across)
    outer_b, own5, passed, inner, d1, d2, d3, d4, d5, s5 = call(
        second_half, [vmem] * 10, [(vmem, states), *kept], [], 20_000_000, 4, {1 + k: 1 + k for k in range(9)}
    )(x_next, *half)
    passed = lax.ppermute(passed, "gz", within)
    outer_b = lax.ppermute(outer_b, "gz", across)
    (own5,) = call(hand_on, [vmem] * 2, [(vmem, arr(2))], [], 5_000_000, 4)(own5, passed)
    outer5 = lax.ppermute(own5, "gz", across)
    inner = lax.ppermute(inner, "gz", within)
    o1, o2, o3, sums_c, limits = call(
        interiors,
        [smem] + [vmem] * 3,
        [(hbm, arr(n)) for n in (32, 16, 8)] + [(vmem, tiles(3)), (vmem, jax.ShapeDtypeStruct((2, 8, 128), f32))],
        [buf(32), buf(16), buf(8), pltpu.SemaphoreType.DMA((6,))],
        20_000_000,
        8,
    )(threshold, d1, d2, d3)
    e1, e2, e3, n4, n5, n6, ends, sums_a = call(
        near,
        [vmem] * 10,
        [(vmem, arr(n)) for n in (3, 3, 3, 4, 2, 2, 2)] + [(vmem, tiles(3))],
        [],
        2_000_000_000,
        4,
    )(limits, d1, d2, d3, d4, d5, s5, inner, own5, sums_c)
    (relayed,) = call(hand_in, [vmem] * 3, [(vmem, arr(2))], [], 5_000_000, 4)(outer_a, outer_b, sums_a)
    received = lax.ppermute(relayed, "gz", within)
    m5, m6, sums_b, o1, o2, o3, o4 = call(
        edges,
        [vmem] * 13 + [hbm] * 3,
        [(vmem, arr(2)), (vmem, arr(2)), (vmem, tiles(4))] + [(hbm, arr(n)) for n in (32, 16, 8, 4)],
        [buf(2), buf(3), buf(3), buf(4), pltpu.SemaphoreType.DMA((14,))],
        1_000_000_000,
        4,
        {13: 3, 14: 4, 15: 5},
    )(limits, outer_a, outer_b, d1, d2, d3, n4, n5, n6, relayed, e1, e2, e3, o1, o2, o3)
    b5, b6, total = call(
        fifth,
        [vmem] * 9,
        [(vmem, arr(2)), (vmem, arr(2)), (vmem, jax.ShapeDtypeStruct((1, 128), f32))],
        [],
        5_000_000,
        4,
    )(limits, outer5, inner, received, m5, m6, ends, sums_a, sums_b)

    devices = count * lax.axis_size("xy")
    parts = lax.all_to_all(jnp.broadcast_to(total, (devices, 1, 128)), ("gz", "xy"), 0, 0, tiled=True)
    cells = np.zeros((1, 128), np.float32) + 1.0
    cells[0, :12] = [n * 32 * 256 * devices for n in (32, 16, 8, 4, 2, 2)] * 2
    o5, o6, energy = call(
        finish,
        [vmem] * 4,
        [(hbm, arr(2)), (hbm, arr(2)), (hbm, jax.ShapeDtypeStruct((2, 6), f32))],
        [pltpu.VMEM((2, 6), f32), pltpu.SemaphoreType.DMA((3,))],
        5_000_000,
        4,
    )(cells, parts, b5, b6)
    return o1, o2, o3, o4, o5, o6, energy


def solution(mesh):
    split = P(None, "gz", "xy", None)

    def step(fields, threshold):
        return local(fields, threshold)

    step = jax.shard_map(step, mesh=mesh, in_specs=(split, P()), out_specs=(split,) * 6 + (P(),), check_vma=False)
    return step
```
